16 devices in a mesh: dp: 2 (over y, z), ep: 8 (over x, core).
Axes of the slice: x: 4, y: 2, z: 1, core: 2. Of those that a mesh axis runs over, the one named last changes fastest.
The devices are a block of a 4x4x8 slice.
Arguments:
- x: bfloat16 [2, 8, 256, 2048], P('dp', 'ep'), parts along dimension 0
- expert: int32 [2, 8, 256, 8], P('dp', 'ep'), parts along dimension 0
- slot: int32 [2, 8, 256, 8], P('dp', 'ep'), parts along dimension 0
- gate: float32 [2, 8, 256, 8], P('dp', 'ep'), parts along dimension 0
- w_gate: bfloat16 [64, 2048, 1024], P('ep')
- w_up: bfloat16 [64, 2048, 1024], P('ep')
- w_down: bfloat16 [64, 1024, 2048], P('ep')
Outputs:
- y: bfloat16 [2, 8, 256, 2048], P('dp', 'ep'), parts along dimension 0
There are 2 independent parts. The reference program is written for one: setup_inputs(seed, part) draws one part's arguments, and reference() takes and returns one part's arrays. A program takes and returns all parts, laid end to end along the dimension named above; an argument that names none is the same for every part.
All inputs are finite; a program needn't handle non-finite values.
Results may differ from the reference program's by a relative error of at most 0.009.
Values are sent between devices in bfloat16 or wider.
A program may use at most 768 MiB of HBM per device.

```python
import jax
import jax.numpy as jnp

MEMBERS = 8
TOKENS = 256
D = 2048
FF = 1024
TOP = 8
EXPERTS = 64
SLOTS = 5 * TOKENS * TOP // (4 * EXPERTS)


def setup_inputs(seed: int = 0, part: int = 0) -> dict:
    own, k1, k2, k3, k4, k5, k6 = jax.random.split(jax.random.key(seed), 7)
    kx, ke, kl, kg = jax.random.split(jax.random.fold_in(own, part), 4)
    devices = (1, MEMBERS)
    place = jax.random.permutation(kl, jnp.arange(EXPERTS, dtype=jnp.uint32))
    slow = ((EXPERTS + (9 * place) % EXPERTS) << ((9 * place) // EXPERTS)) // EXPERTS
    wait = (jax.random.bits(ke, (*devices, TOKENS, EXPERTS), jnp.uint32) >> 10) * slow
    expert = jnp.argsort(wait, axis=-1)[..., :TOP].astype(jnp.int32)
    chosen = jax.nn.one_hot(expert, EXPERTS, dtype=jnp.int32)
    in_line = jnp.cumsum(chosen.reshape(*devices, TOKENS * TOP, EXPERTS), axis=2) - 1
    slot = jnp.sum(in_line.reshape(chosen.shape) * chosen, axis=-1)

    def one(key, rows, columns):
        return (jax.random.normal(key, (rows, columns), jnp.float32) * rows**-0.5).astype(jnp.bfloat16)

    def weights(key, rows, columns):
        return jax.lax.map(lambda k: one(k, rows, columns), jax.random.split(key, EXPERTS))

    return {
        "x": jax.random.normal(kx, (*devices, TOKENS, D), jnp.float32).astype(jnp.bfloat16),
        "expert": expert,
        "slot": slot,
        "gate": jax.nn.softmax(jax.random.normal(kg, expert.shape, jnp.float32)),
        "w_gate": weights(k1, D, FF),
        "w_up": weights(k2, D, FF),
        "w_down": weights(k3, FF, D),
    }


def einsum(form, a, b):
    return jnp.einsum(form, a.astype(jnp.float32), b.astype(jnp.float32))


def reference(x, expert, slot, gate, w_gate, w_up, w_down):
    to_expert = jax.nn.one_hot(expert, EXPERTS, dtype=jnp.bfloat16)
    to_slot = jax.nn.one_hot(slot, SLOTS, dtype=jnp.bfloat16)
    weighted = to_expert * gate[..., None].astype(jnp.bfloat16)
    dispatch = einsum("abtke,abtkc->abtec", to_expert, to_slot).astype(jnp.bfloat16)
    combine = einsum("abtke,abtkc->abtec", weighted, to_slot).astype(jnp.bfloat16)
    z = einsum("abtec,abtd->aebcd", dispatch, x).astype(jnp.bfloat16)
    h = jax.nn.silu(einsum("aebcd,edf->aebcf", z, w_gate))
    h = (h * einsum("aebcd,edf->aebcf", z, w_up)).astype(jnp.bfloat16)
    out = einsum("aebcf,efd->aebcd", h, w_down).astype(jnp.bfloat16)
    y = einsum("abtec,aebcd->abtd", combine, out)
    return y.astype(jnp.bfloat16)
```

```python
import functools

import jax
import jax.numpy as jnp
from jax import lax
from jax.experimental import pallas as pl
from jax.experimental.pallas import tpu as pltpu
from jax.sharding import PartitionSpec as P

MESH = pl.DeviceIdType.MESH
F32, BF16 = jnp.float32, jnp.bfloat16
GROUPS = ((0, 1), (2, 3), (4, 5), (6,), (7,))
AHEAD = 2
RING = 4
RING2 = 8


def kernel(
    n, slots,
    x_hbm, ex, sl, ga, wg_hbm, wu_hbm, wd_hbm, y_hbm,
    xall, accg, accu, z, h, disp, comb, wgb, wub, wdb, outs, me_e, me_s, me_g, pr, r1, r2,
    x_sem, wg_sem, wu_sem, wd_sem, y_sem, ms_sem, mr_sem, as_sem, ar_sem, ss_sem, sr_sem,
):
    experts = wg_hbm.shape[0]
    tokens, model = x_hbm.shape
    ff = wg_hbm.shape[2]
    top = ex.shape[0]
    rows = experts * slots
    chunks, _, _, width = xall.shape
    half = tokens // 2
    chips = n // 2
    me = lax.axis_index("ep")
    chip, core = me // 2, me % 2
    other = 1 - core
    lchip, rchip, ochip = (chip + chips - 1) % chips, (chip + 1) % chips, (chip + 2) % chips
    left, right, opp, partner = 2 * lchip + core, 2 * rchip + core, 2 * ochip + core, 2 * chip + other

    def rcopy(src, dst, ssem, rsem, dev):
        return pltpu.make_async_remote_copy(
            src_ref=src, dst_ref=dst, send_sem=ssem, recv_sem=rsem,
            device_id={"ep": dev}, device_id_type=MESH,
        )

    def xload(j):
        return pltpu.make_async_copy(x_hbm.at[:, pl.ds(j * width, width)], xall.at[j, me], x_sem.at[j])

    for j in range(chunks):
        xload(j).start()

    def wload(g, e, slot):
        k0, kk = GROUPS[g][0] * width, len(GROUPS[g]) * width
        return [
            pltpu.make_async_copy(w.at[e, pl.ds(k0, kk), :], b.at[slot, pl.ds(0, kk), :], s.at[slot])
            for w, b, s in ((wg_hbm, wgb, wg_sem), (wu_hbm, wub, wu_sem))
        ]

    def dload(c, e, slot):
        return pltpu.make_async_copy(wd_hbm.at[e, :, pl.ds(c * width, width)], wdb.at[slot], wd_sem.at[slot])

    for e in range(RING):
        for c in wload(0, e, e):
            c.start()

    barrier = pltpu.get_barrier_semaphore()
    for o in range(1, n):
        pl.semaphore_signal(barrier, inc=1, device_id={"ep": (me + o) % n}, device_id_type=MESH)
    pl.semaphore_wait(barrier, n - 1)

    def own(j):
        return [
            rcopy(xall.at[j, me], xall.at[j, me], as_sem.at[0, j], ar_sem.at[0, j], right),
            rcopy(xall.at[j, me], xall.at[j, me], as_sem.at[1, j], ar_sem.at[1, j], left),
            rcopy(xall.at[j, me], xall.at[j, me], as_sem.at[2, j], ar_sem.at[4, j], partner),
        ]

    def forward(j):
        lo, hi = pl.ds(0, half), pl.ds(half, half)
        return [
            rcopy(xall.at[j, left, lo], xall.at[j, left, lo], as_sem.at[3, j], ar_sem.at[2, j], right),
            rcopy(xall.at[j, right, hi], xall.at[j, right, hi], as_sem.at[4, j], ar_sem.at[3, j], left),
            rcopy(xall.at[j, left], xall.at[j, left], as_sem.at[5, j], ar_sem.at[5, j], partner),
            rcopy(xall.at[j, right], xall.at[j, right], as_sem.at[6, j], ar_sem.at[6, j], partner),
        ]

    def across(j):
        return [rcopy(xall.at[j, opp], xall.at[j, opp], as_sem.at[7, j], ar_sem.at[7, j], partner)]

    def got(dst, sem):
        rcopy(dst, dst, sem, sem, partner).wait_recv()

    def send_own(j):
        xload(j).wait()
        for c in own(j):
            c.start()

    def step_a(j):
        got(xall.at[j, left], ar_sem.at[0, j])
        got(xall.at[j, right], ar_sem.at[1, j])
        for c in forward(j):
            c.start()
        if j + AHEAD < chunks:
            send_own(j + AHEAD)

    def step_b(j):
        got(xall.at[j, opp, pl.ds(0, half)], ar_sem.at[2, j])
        got(xall.at[j, opp, pl.ds(half, half)], ar_sem.at[3, j])
        for c in across(j):
            c.start()

    def step_c(j):
        for i, q in enumerate((chip, lchip, rchip, ochip)):
            got(xall.at[j, 2 * q + other], ar_sem.at[4 + i, j])

    for j in range(AHEAD):
        send_own(j)

    def meta(o):
        to = (me + o) % n
        return [
            rcopy(src, dst.at[me], ms_sem.at[i, o - 1], mr_sem.at[i, o - 1], to)
            for i, (src, dst) in enumerate(((ex, me_e), (sl, me_s), (ga, me_g)))
        ]

    for o in range(1, n):
        for c in meta(o):
            c.start()
    me_e[me] = ex[...]
    me_s[me] = sl[...]
    me_g[me] = ga[...]
    for e in range(RING2):
        dload(0, e, e).start()
    for o in range(1, n):
        source = (me + n - o) % n
        for i, dst in enumerate((me_e, me_s, me_g)):
            got(dst.at[source], mr_sem.at[i, o - 1])

    def tables(s, _):
        e, c, g = me_e[s], me_s[s], me_g[s]
        local = e - experts * me
        ok = (local >= 0) & (local < experts) & (c < slots)
        code = jnp.where(ok, local * slots + c, -1)
        for r0 in range(0, rows, 128):
            size = min(128, rows - r0)
            row = r0 + lax.broadcasted_iota(jnp.int32, (size, tokens), 0)
            w = jnp.zeros((size, tokens), F32)
            d = jnp.zeros((size, tokens), F32)
            for k in range(top):
                hit = row == code[k : k + 1, :]
                w = jnp.where(hit, g[k : k + 1, :], w)
                d = jnp.where(hit, 1.0, d)
            disp[s, r0 : r0 + size, :] = d.astype(BF16)
            comb[s, :, r0 : r0 + size] = w.T.astype(BF16)
        return _

    lax.fori_loop(0, n, tables, 0)

    def dispatch(j, k0):
        def pair(q, _):
            a = jnp.dot(disp[2 * q], xall[j, 2 * q], preferred_element_type=F32)
            b = jnp.dot(disp[2 * q + 1], xall[j, 2 * q + 1], preferred_element_type=F32)
            at = pl.ds(pl.multiple_of(q * 2 * slots, 16), 2 * slots)
            for e in range(experts):
                part = slice(e * slots, (e + 1) * slots)
                z[e, at, k0 : k0 + width] = jnp.concatenate([a[part], b[part]], 0).astype(BF16)
            return _

        lax.fori_loop(0, chips, pair, 0)

    def gemm1(g, e0, e1):
        kk = len(GROUPS[g]) * width
        first, last = g == 0, g == len(GROUPS) - 1

        def one(e, _):
            slot = e % RING
            for c in wload(g, e, slot):
                c.wait()
            lhs = z[e, :, :kk]
            for f0 in range(0, ff, width):
                f = slice(f0, f0 + width)
                gg = jnp.dot(lhs, wgb[slot, :kk, f], preferred_element_type=F32)
                uu = jnp.dot(lhs, wub[slot, :kk, f], preferred_element_type=F32)
                if not first:
                    gg += accg[e, :, f]
                    uu += accu[e, :, f]
                if last:
                    h[e, :, f] = (gg * jax.nn.sigmoid(gg) * uu).astype(BF16)
                else:
                    accg[e, :, f] = gg
                    accu[e, :, f] = uu
            if e1 + RING <= experts:
                for c in wload(g, e + RING, slot):
                    c.start()
            elif not last:
                for c in wload(g + 1, e + RING - experts, slot):
                    c.start()
            return _

        lax.fori_loop(e0, e1, one, 0)

    mid = experts // 2
    before = (
        lambda: (step_a(0), step_a(1), step_b(0), step_a(2), step_b(1), step_c(0), step_c(1)),
        lambda: (step_a(4), step_b(3), step_c(2), step_c(3)),
        lambda: (step_a(6), step_b(5), step_c(4), step_c(5)),
        lambda: (step_c(6),),
        lambda: (step_c(7),),
    )
    within = (
        lambda: (step_a(3), step_b(2)),
        lambda: (step_a(5), step_b(4)),
        lambda: (step_a(7), step_b(6)),
        lambda: (step_b(7),),
        lambda: (),
    )
    for g, js in enumerate(GROUPS):
        before[g]()
        for i, j in enumerate(js):
            dispatch(j, i * width)
        gemm1(g, 0, mid)
        within[g]()
        gemm1(g, mid, experts)

    for o in range(1, n):
        for c in meta(o):
            c.wait_send()
    for j in range(chunks):
        for c in own(j) + forward(j) + across(j):
            c.wait_send()

    keep = lambda c, q: accg.at[c, pl.ds(0, tokens), pl.ds(pl.multiple_of(q * width, width), width)]

    def die(c):
        return rcopy(xall.at[c, pl.ds(0, chips)], pr.at[c], ss_sem.at[0, c], sr_sem.at[0, c], partner)

    lo, hi = pl.ds(0, half), pl.ds(half, half)

    def far(c):
        return [
            rcopy(xall.at[c, chips, lo], r1.at[c, 0], ss_sem.at[1, c], sr_sem.at[1, c], right),
            rcopy(xall.at[c, chips, hi], r1.at[c, 1], ss_sem.at[2, c], sr_sem.at[2, c], left),
        ]

    def near(c):
        return [
            rcopy(xall.at[c, chips + 1, hi], r2.at[c, 0, hi], ss_sem.at[3, c], sr_sem.at[3, c], right),
            rcopy(xall.at[c, chips + 2, lo], r2.at[c, 1, lo], ss_sem.at[4, c], sr_sem.at[4, c], left),
        ]

    def merged(c):
        return [
            rcopy(xall.at[c, chips + 1, lo], r2.at[c, 0, lo], ss_sem.at[5, c], sr_sem.at[5, c], right),
            rcopy(xall.at[c, chips + 2, hi], r2.at[c, 1, hi], ss_sem.at[6, c], sr_sem.at[6, c], left),
        ]

    def store(c):
        return pltpu.make_async_copy(
            xall.at[c, chips + 3], y_hbm.at[:, pl.ds(pl.multiple_of(c * width, width), width)], y_sem.at[c]
        )

    def both(c, q, at):
        return keep(c, q)[at] + pr[c, q, at].astype(F32)

    def compute(c):
        def pair(i, _):
            pieces = []
            for b in range(2):
                e = 2 * i + b
                dload(c, e, e % RING2).wait()
                pieces.append(jnp.dot(h[e], wdb[e % RING2], preferred_element_type=F32))
            at = pl.ds(pl.multiple_of(i * 2 * slots, 16), 2 * slots)
            for s in range(n):
                part = slice(s * slots, (s + 1) * slots)
                outs[s, at, :] = jnp.concatenate([v[part] for v in pieces], 0).astype(BF16)

            @pl.when(c + 1 < chunks)
            def _next():
                for b in range(2):
                    e = 2 * i + b
                    dload(c + 1, e, e % RING2).start()

            return _

        lax.fori_loop(0, experts // 2, pair, 0)
        for q in range(chips):
            s = 2 * q + other
            xall[c, q] = jnp.dot(comb[s], outs[s], preferred_element_type=F32).astype(BF16)
        die(c).start()
        for q in range(chips):
            s = 2 * q + core
            keep(c, q)[...] = jnp.dot(comb[s], outs[s], preferred_element_type=F32)

    def stage1(c):
        die(c).wait_recv()
        xall[c, chips] = both(c, ochip, pl.ds(0, tokens)).astype(BF16)
        xall[c, chips + 1, hi] = both(c, rchip, hi).astype(BF16)
        xall[c, chips + 2, lo] = both(c, lchip, lo).astype(BF16)
        for k in far(c) + near(c):
            k.start()

    def stage2(c):
        for k in far(c):
            k.wait_recv()
        xall[c, chips + 1, lo] = (both(c, rchip, lo) + r1[c, 0].astype(F32)).astype(BF16)
        xall[c, chips + 2, hi] = (both(c, lchip, hi) + r1[c, 1].astype(F32)).astype(BF16)
        for k in merged(c):
            k.start()

    def stage3(c):
        for k in near(c) + merged(c):
            k.wait_recv()
        total = both(c, chip, pl.ds(0, tokens)) + r2[c, 0].astype(F32) + r2[c, 1].astype(F32)
        xall[c, chips + 3] = total.astype(BF16)
        store(c).start()

    def round_(t, _):
        for lag, stage in enumerate((compute, stage1, stage2, stage3)):
            pl.when((t >= lag) & (t < chunks + lag))(functools.partial(stage, t - lag))
        return _

    lax.fori_loop(0, chunks + 3, round_, 0)

    def drain(c, _):
        die(c).wait_send()
        for k in far(c) + near(c) + merged(c):
            k.wait_send()
        store(c).wait()
        return _

    lax.fori_loop(0, chunks, drain, 0)


def solution(mesh):
    n = mesh.shape["ep"]

    def local(x, expert, slot, gate, w_gate, w_up, w_down):
        tokens, model = x.shape[2:]
        top = expert.shape[3]
        experts, _, ff = w_gate.shape
        slots = 5 * tokens * top // (4 * experts * n)
        rows = experts * slots
        width = 256
        chunks = model // width
        flat = lambda v: v.reshape(tokens, top).T
        vmem = pltpu.VMEM
        dma = pltpu.SemaphoreType.DMA
        any_, inv = pl.BlockSpec(memory_space=pl.ANY), pl.BlockSpec(memory_space=pltpu.VMEM)
        flops = 6 * n * rows * model * ff
        y = pl.pallas_call(
            functools.partial(kernel, n, slots),
            out_shape=jax.ShapeDtypeStruct((tokens, model), BF16),
            in_specs=[any_, inv, inv, inv, any_, any_, any_],
            out_specs=any_,
            scratch_shapes=[
                vmem((chunks, n, tokens, width), BF16),
                vmem((experts, n * slots, ff), F32),
                vmem((experts, n * slots, ff), F32),
                vmem((experts, n * slots, 2 * width), BF16),
                vmem((experts, n * slots, ff), BF16),
                vmem((n, rows, tokens), BF16),
                vmem((n, tokens, rows), BF16),
                vmem((RING, 2 * width, ff), BF16),
                vmem((RING, 2 * width, ff), BF16),
                vmem((RING2, ff, width), BF16),
                vmem((n, rows, width), BF16),
                vmem((n, top, tokens), jnp.int32),
                vmem((n, top, tokens), jnp.int32),
                vmem((n, top, tokens), F32),
                vmem((chunks, n // 2, tokens, width), BF16),
                vmem((chunks, 2, tokens // 2, width), BF16),
                vmem((chunks, 2, tokens, width), BF16),
                dma((chunks,)),
                dma((RING,)),
                dma((RING,)),
                dma((RING2,)),
                dma((chunks,)),
                dma((3, n - 1)),
                dma((3, n - 1)),
                dma((8, chunks)),
                dma((8, chunks)),
                dma((7, chunks)),
                dma((7, chunks)),
            ],
            compiler_params=pltpu.CompilerParams(
                collective_id=0, has_side_effects=True, vmem_limit_bytes=67_000_000
            ),
            cost_estimate=pl.CostEstimate(
                flops=flops, bytes_accessed=6 * experts * model * ff, transcendentals=n * rows * ff
            ),
            name="moe",
        )(x.reshape(tokens, model), flat(expert), flat(slot), flat(gate), w_gate, w_up, w_down)
        return y.reshape(x.shape)

    token, weight = P("dp", "ep", None, None), P("ep", None, None)
    return jax.shard_map(
        local,
        mesh=mesh,
        in_specs=(token,) * 4 + (weight,) * 3,
        out_specs=token,
        check_vma=False,
    )
```

```python
import functools

import jax
import jax.numpy as jnp
from jax import lax
from jax.experimental import pallas as pl
from jax.experimental.pallas import tpu as pltpu
from jax.sharding import PartitionSpec as P

MESH = pl.DeviceIdType.MESH
F32, BF16 = jnp.float32, jnp.bfloat16
GROUPS = ((0,), (1, 2), (3, 4), (5, 6), (7,))
DOWN = (1, 2, 2, 2, 1)
AHEAD = 2
RING = 4
PAD = 128


def kernel(
    n, slots, width,
    x_hbm, ex, sl, ga, wg_hbm, wu_hbm, wd_hbm, y_hbm,
    xall, accg, accu, z, h, disp, comb, wgb, wub, wdb, me_c, me_g, pr, r1, r2,
    x_sem, wg_sem, wu_sem, wd_sem, y_sem, ms_sem, mr_sem, as_sem, ar_sem, ss_sem, sr_sem,
):
    experts = wg_hbm.shape[0]
    tokens = x_hbm.shape[0]
    ff = wg_hbm.shape[2]
    top = ex.shape[0]
    rows = experts * slots
    chunks = xall.shape[0]
    half = tokens // 2
    chips = n // 2
    me = lax.axis_index("ep")
    chip, core = me // 2, me % 2
    other = 1 - core
    lchip, rchip, ochip = (chip + chips - 1) % chips, (chip + 1) % chips, (chip + 2) % chips
    left, right, opp, partner = 2 * lchip + core, 2 * rchip + core, 2 * ochip + core, 2 * chip + other
    others = tuple(2 * q + other for q in (chip, lchip, rchip, ochip))

    def rcopy(src, dst, ssem, rsem, dev):
        return pltpu.make_async_remote_copy(
            src_ref=src, dst_ref=dst, send_sem=ssem, recv_sem=rsem,
            device_id={"ep": dev}, device_id_type=MESH,
        )

    def go(copies):
        for c in copies:
            c.start()

    def got(dst, sem):
        rcopy(dst, dst, sem, sem, partner).wait_recv()

    def xload(j):
        return pltpu.make_async_copy(x_hbm.at[:, pl.ds(j * width, width)], xall.at[j, me], x_sem.at[j])

    go([xload(j) for j in range(chunks)])

    def wload(g, e, slot):
        k0, kk = GROUPS[g][0] * width, len(GROUPS[g]) * width
        return [
            pltpu.make_async_copy(
                w.at[e, pl.ds(k0, kk), :], b.at[slot, pl.ds(0, kk), pl.ds(0, ff)], s.at[slot]
            )
            for w, b, s in ((wg_hbm, wgb, wg_sem), (wu_hbm, wub, wu_sem))
        ]

    def dload(c0, nc, e, slot):
        cols = pl.ds(pl.multiple_of(c0 * width, width), nc * width)
        return pltpu.make_async_copy(
            wd_hbm.at[e, :, cols], wdb.at[slot, :, pl.ds(0, nc * width)], wd_sem.at[slot]
        )

    for e in range(RING):
        go(wload(0, e, e))
    go([dload(0, DOWN[0], e, e) for e in range(RING)])

    barrier = pltpu.get_barrier_semaphore()
    for p in (left, right, partner):
        pl.semaphore_signal(barrier, inc=1, device_id={"ep": p}, device_id_type=MESH)
    me_c[me] = jnp.where(sl[...] < slots, ex[...] * slots + sl[...], -1)
    me_g[me] = ga[...]
    pl.semaphore_wait(barrier, 3)

    def table(i, r, s, dev):
        return [
            rcopy(t.at[s], t.at[s], ms_sem.at[k, i], mr_sem.at[k, r], dev) for k, t in enumerate((me_c, me_g))
        ]

    def tgot(r, s):
        for k, t in enumerate((me_c, me_g)):
            got(t.at[s], mr_sem.at[k, r])

    t_own = table(0, 0, me, right) + table(1, 1, me, left) + table(2, 4, me, partner)
    t_next = table(3, 2, left, right) + table(4, 5, left, partner) + table(5, 6, right, partner)
    t_last = table(6, 7, opp, partner)

    def own(j):
        return [
            rcopy(xall.at[j, me], xall.at[j, me], as_sem.at[0, j], ar_sem.at[0, j], right),
            rcopy(xall.at[j, me], xall.at[j, me], as_sem.at[1, j], ar_sem.at[1, j], left),
            rcopy(xall.at[j, me], xall.at[j, me], as_sem.at[2, j], ar_sem.at[4, j], partner),
        ]

    lo, hi = pl.ds(0, half), pl.ds(half, half)

    def forward(j):
        return [
            rcopy(xall.at[j, left, lo], xall.at[j, left, lo], as_sem.at[3, j], ar_sem.at[2, j], right),
            rcopy(xall.at[j, right, hi], xall.at[j, right, hi], as_sem.at[4, j], ar_sem.at[3, j], left),
            rcopy(xall.at[j, left], xall.at[j, left], as_sem.at[5, j], ar_sem.at[5, j], partner),
            rcopy(xall.at[j, right], xall.at[j, right], as_sem.at[6, j], ar_sem.at[6, j], partner),
        ]

    def across(j):
        return [rcopy(xall.at[j, opp], xall.at[j, opp], as_sem.at[7, j], ar_sem.at[7, j], partner)]

    def send_own(j):
        xload(j).wait()
        go(own(j))

    def step_a(j):
        got(xall.at[j, left], ar_sem.at[0, j])
        got(xall.at[j, right], ar_sem.at[1, j])
        go(forward(j))
        if j + AHEAD < chunks:
            send_own(j + AHEAD)

    def step_b(j):
        got(xall.at[j, opp, lo], ar_sem.at[2, j])
        got(xall.at[j, opp, hi], ar_sem.at[3, j])
        go(across(j))

    def step_c(j):
        for i, s in enumerate(others):
            got(xall.at[j, s], ar_sem.at[4 + i, j])

    A, B, C = (functools.partial(functools.partial, f) for f in (step_a, step_b, step_c))

    go(t_own)
    for j in range(AHEAD):
        send_own(j)
    tgot(0, left)
    tgot(1, right)
    go(t_next)
    tgot(2, opp)
    go(t_last)
    step_a(0)
    for i, s in enumerate(others):
        tgot(4 + i, s)

    def tables(s, _):
        code, g = me_c[s] - rows * me, me_g[s]
        for r0 in range(0, rows, 128):
            size = min(128, rows - r0)
            row = r0 + lax.broadcasted_iota(jnp.int32, (size, tokens), 0)
            w = jnp.zeros((size, tokens), F32)
            d = jnp.zeros((size, tokens), F32)
            for k in range(top):
                hit = row == code[k : k + 1, :]
                w = jnp.where(hit, g[k : k + 1, :], w)
                d = jnp.where(hit, 1.0, d)
            disp[s, r0 : r0 + size, :] = d.astype(BF16)
            comb[s, :, r0 : r0 + size] = w.T.astype(BF16)
        return _

    lax.fori_loop(0, n - 2, tables, 0)
    step_a(1)
    lax.fori_loop(n - 2, n, tables, 0)

    def dispatch(j, k0):
        for q in range(chips):
            a = jnp.dot(disp[2 * q], xall[j, 2 * q], preferred_element_type=F32)
            b = jnp.dot(disp[2 * q + 1], xall[j, 2 * q + 1], preferred_element_type=F32)
            at = slice(q * 2 * slots, (q + 1) * 2 * slots)
            for e in range(experts):
                part = slice(e * slots, (e + 1) * slots)
                z[e, at, k0 : k0 + width] = jnp.concatenate([a[part], b[part]], 0).astype(BF16)

    def gemm1(g, hooks):
        kk = len(GROUPS[g]) * width
        first, last = g == 0, g == len(GROUPS) - 1

        def one(e, _):
            for at, hook in hooks:
                pl.when(e == at)(hook)
            slot = e % RING
            for c in wload(g, e, slot):
                c.wait()
            lhs = z[e, :, :kk]
            for f0 in range(0, ff, width):
                f = slice(f0, f0 + width)
                gg = jnp.dot(lhs, wgb[slot, :kk, f], preferred_element_type=F32)
                uu = jnp.dot(lhs, wub[slot, :kk, f], preferred_element_type=F32)
                if not first:
                    gg += accg[e, :, f]
                    uu += accu[e, :, f]
                if last:
                    h[e, :, f] = (gg * jax.nn.sigmoid(gg) * uu).astype(BF16)
                else:
                    accg[e, :, f] = gg
                    accu[e, :, f] = uu
            pl.when(e + RING < experts)(lambda: go(wload(g, e + RING, slot)))
            if not last:
                pl.when(e + RING >= experts)(lambda: go(wload(g + 1, e + RING - experts, slot)))
            return _

        lax.fori_loop(0, experts, one, 0)

    before = (
        (B(0), C(0)),
        (A(3), B(2), C(1), C(2)),
        (A(5), B(4), C(3), C(4)),
        (A(7), B(6), C(5), C(6)),
        (C(7),),
    )
    within = (
        ((3, A(2)), (6, B(1))),
        ((2, A(4)), (4, B(3))),
        ((2, A(6)), (4, B(5))),
        ((2, B(7)),),
        (),
    )
    for g, js in enumerate(GROUPS):
        for f in before[g]:
            f()
        for i, j in enumerate(js):
            dispatch(j, i * width)
        gemm1(g, within[g])

    for c in t_own + t_next + t_last:
        c.wait_send()
    for j in range(chunks):
        for c in own(j) + forward(j) + across(j):
            c.wait_send()

    keep = lambda c, q: accg.at[c, pl.ds(0, tokens), pl.ds(pl.multiple_of(q * width, width), width)]

    def die(c):
        return rcopy(xall.at[c, pl.ds(0, chips)], pr.at[c], ss_sem.at[0, c], sr_sem.at[0, c], partner)

    def far(c):
        return [
            rcopy(xall.at[c, chips, lo], r1.at[c, 0], ss_sem.at[1, c], sr_sem.at[1, c], right),
            rcopy(xall.at[c, chips, hi], r1.at[c, 1], ss_sem.at[2, c], sr_sem.at[2, c], left),
        ]

    def near(c):
        return [
            rcopy(xall.at[c, chips + 1, hi], r2.at[c, 0, hi], ss_sem.at[3, c], sr_sem.at[3, c], right),
            rcopy(xall.at[c, chips + 2, lo], r2.at[c, 1, lo], ss_sem.at[4, c], sr_sem.at[4, c], left),
        ]

    def merged(c):
        return [
            rcopy(xall.at[c, chips + 1, lo], r2.at[c, 0, lo], ss_sem.at[5, c], sr_sem.at[5, c], right),
            rcopy(xall.at[c, chips + 2, hi], r2.at[c, 1, hi], ss_sem.at[6, c], sr_sem.at[6, c], left),
        ]

    def store(c):
        return pltpu.make_async_copy(
            xall.at[c, chips + 3], y_hbm.at[:, pl.ds(pl.multiple_of(c * width, width), width)], y_sem.at[c]
        )

    def both(c, q, at):
        return keep(c, q)[at] + pr[c, q, at].astype(F32)

    def stage1(c):
        die(c).wait_recv()
        xall[c, chips] = both(c, ochip, pl.ds(0, tokens)).astype(BF16)
        xall[c, chips + 1, hi] = both(c, rchip, hi).astype(BF16)
        xall[c, chips + 2, lo] = both(c, lchip, lo).astype(BF16)
        go(far(c) + near(c))

    def stage2(c):
        for k in far(c):
            k.wait_recv()
        xall[c, chips + 1, lo] = (both(c, rchip, lo) + r1[c, 0].astype(F32)).astype(BF16)
        xall[c, chips + 2, hi] = (both(c, lchip, hi) + r1[c, 1].astype(F32)).astype(BF16)
        go(merged(c))

    def stage3(c):
        for k in near(c) + merged(c):
            k.wait_recv()
        total = both(c, chip, pl.ds(0, tokens)) + r2[c, 0].astype(F32) + r2[c, 1].astype(F32)
        xall[c, chips + 3] = total.astype(BF16)
        store(c).start()

    def down(c0, nc, after, hooks):
        cols = nc * width

        def pair(i, _):
            for at, hook in hooks:
                pl.when(i == at)(hook)
            pieces = []
            for b in range(2):
                slot = (2 * i + b) % RING
                dload(c0, nc, 2 * i + b, slot).wait()
                pieces.append(
                    jnp.dot(h[2 * i + b, :, :ff], wdb[slot, :, :cols], preferred_element_type=F32)
                )
            at = pl.ds(pl.multiple_of(i * 2 * slots, 16), 2 * slots)
            for s in range(n):
                part = slice(s * slots, (s + 1) * slots)
                z[s, at, :cols] = jnp.concatenate([v[part] for v in pieces], 0).astype(BF16)
            for b in range(2):
                e = 2 * i + b + RING
                pl.when(e < experts)(lambda: dload(c0, nc, e, e % RING).start())
                pl.when(e >= experts)(lambda: after(e - experts, e % RING))
            return _

        lax.fori_loop(0, experts // 2, pair, 0)
        for k in range(nc):
            col = slice(k * width, (k + 1) * width)
            for q in range(chips):
                s = 2 * q + other
                xall[c0 + k, q] = jnp.dot(comb[s], z[s, :, col], preferred_element_type=F32).astype(BF16)
            die(c0 + k).start()
        for k in range(nc):
            col = slice(k * width, (k + 1) * width)
            for q in range(chips):
                s = 2 * q + core
                keep(c0 + k, q)[...] = jnp.dot(comb[s], z[s, :, col], preferred_element_type=F32)

    def stages(*todo):
        for f, c in todo:
            f(c)

    down(0, 1, lambda e, slot: dload(1, 2, e, slot).start(), ())

    def middle(r, _):
        c = 2 * r - 1
        more = r < 3

        def after(e, slot):
            pl.when(more)(lambda: dload(c + 2, 2, e, slot).start())
            pl.when(jnp.logical_not(more))(lambda: dload(chunks - 1, 1, e, slot).start())

        def one():
            pl.when(r > 1)(lambda: stage1(c - 2))
            stage1(c - 1)

        def two():
            pl.when(r > 1)(lambda: stage2(c - 2))

        down(c, 2, after, ((1, one), (3, two)))
        stage2(c - 1)
        pl.when(r > 1)(lambda: stages((stage3, c - 3), (stage3, c - 2)))
        return _

    lax.fori_loop(1, 4, middle, 0)
    c = chunks - 1
    down(
        c, 1, lambda e, slot: None,
        ((1, lambda: stages((stage1, c - 2), (stage1, c - 1))), (3, lambda: stages((stage2, c - 2)))),
    )
    stages((stage1, c), (stage2, c - 1), (stage3, c - 3), (stage2, c), (stage3, c - 2), (stage3, c - 1), (stage3, c))

    def drain(c, _):
        die(c).wait_send()
        for k in far(c) + near(c) + merged(c):
            k.wait_send()
        store(c).wait()
        return _

    lax.fori_loop(0, chunks, drain, 0)


def solution(mesh):
    n = mesh.shape["ep"]

    def local(x, expert, slot, gate, w_gate, w_up, w_down):
        tokens, model = x.shape[2:]
        top = expert.shape[3]
        experts, _, ff = w_gate.shape
        slots = 5 * tokens * top // (4 * experts * n)
        rows = experts * slots
        width = 256
        chunks = model // width
        flat = lambda v: v.reshape(tokens, top).T
        vmem = pltpu.VMEM
        dma = pltpu.SemaphoreType.DMA
        any_, inv = pl.BlockSpec(memory_space=pl.ANY), pl.BlockSpec(memory_space=pltpu.VMEM)
        flops = 6 * n * rows * model * ff
        y = pl.pallas_call(
            functools.partial(kernel, n, slots, width),
            out_shape=jax.ShapeDtypeStruct((tokens, model), BF16),
            in_specs=[any_, inv, inv, inv, any_, any_, any_],
            out_specs=any_,
            scratch_shapes=[
                vmem((chunks, n, tokens, width), BF16),
                vmem((experts, n * slots, ff + PAD), F32),
                vmem((experts, n * slots, ff + PAD), F32),
                vmem((n, rows, 2 * width + PAD), BF16),
                vmem((experts, n * slots, ff + PAD), BF16),
                vmem((n, rows, tokens), BF16),
                vmem((n, tokens, rows), BF16),
                vmem((RING, 2 * width, ff + PAD), BF16),
                vmem((RING, 2 * width, ff + PAD), BF16),
                vmem((RING, ff, 2 * width + PAD), BF16),
                vmem((n, top, tokens), jnp.int32),
                vmem((n, top, tokens), F32),
                vmem((chunks, n // 2, tokens, width), BF16),
                vmem((chunks, 2, tokens // 2, width), BF16),
                vmem((chunks, 2, tokens, width), BF16),
                dma((chunks,)),
                dma((RING,)),
                dma((RING,)),
                dma((RING,)),
                dma((chunks,)),
                dma((2, 7)),
                dma((2, 8)),
                dma((8, chunks)),
                dma((8, chunks)),
                dma((7, chunks)),
                dma((7, chunks)),
            ],
            compiler_params=pltpu.CompilerParams(
                collective_id=0, has_side_effects=True, vmem_limit_bytes=67_000_000
            ),
            cost_estimate=pl.CostEstimate(
                flops=flops, bytes_accessed=6 * experts * model * ff, transcendentals=n * rows * ff
            ),
            name="moe",
        )(x.reshape(tokens, model), flat(expert), flat(slot), flat(gate), w_gate, w_up, w_down)
        return y.reshape(x.shape)

    token, weight = P("dp", "ep", None, None), P("ep", None, None)
    return jax.shard_map(
        local,
        mesh=mesh,
        in_specs=(token,) * 4 + (weight,) * 3,
        out_specs=token,
        check_vma=False,
    )
```

```python
import functools

import jax
import jax.numpy as jnp
from jax import lax
from jax.experimental import pallas as pl
from jax.experimental.pallas import tpu as pltpu
from jax.sharding import PartitionSpec as P

MESH = pl.DeviceIdType.MESH
F32, BF16 = jnp.float32, jnp.bfloat16
GROUPS = ((0,), (1,), (2,), (3,), (4,), (5,), (6, 7))
AHEAD = 2
RING = 4


def kernel(
    n, slots, width,
    x_hbm, ex, sl, ga, wg_hbm, wu_hbm, wd_hbm, y_hbm,
    xall, accg, accu, z, h, disp, comb, wgb, wub, wdb, me_c, me_g, pr, r1, r2,
    x_sem, wg_sem, wu_sem, wd_sem, y_sem, ms_sem, mr_sem, as_sem, ar_sem, ss_sem, sr_sem,
):
    experts = wg_hbm.shape[0]
    tokens = x_hbm.shape[0]
    ff = wg_hbm.shape[2]
    top = ex.shape[0]
    rows = experts * slots
    chunks = xall.shape[0]
    half = tokens // 2
    chips = n // 2
    me = lax.axis_index("ep")
    chip, core = me // 2, me % 2
    other = 1 - core
    lchip, rchip, ochip = (chip + chips - 1) % chips, (chip + 1) % chips, (chip + 2) % chips
    left, right, opp, partner = 2 * lchip + core, 2 * rchip + core, 2 * ochip + core, 2 * chip + other
    others = tuple(2 * q + other for q in (chip, lchip, rchip, ochip))

    def rcopy(src, dst, ssem, rsem, dev):
        return pltpu.make_async_remote_copy(
            src_ref=src, dst_ref=dst, send_sem=ssem, recv_sem=rsem,
            device_id={"ep": dev}, device_id_type=MESH,
        )

    def go(copies):
        for c in copies:
            c.start()

    def got(dst, sem):
        rcopy(dst, dst, sem, sem, partner).wait_recv()

    def xload(j):
        return pltpu.make_async_copy(x_hbm.at[:, pl.ds(j * width, width)], xall.at[j, me], x_sem.at[j])

    go([xload(j) for j in range(chunks)])

    def wload(g, e, slot):
        k0, kk = GROUPS[g][0] * width, len(GROUPS[g]) * width
        return [
            pltpu.make_async_copy(
                w.at[e, pl.ds(k0, kk), :], b.at[slot, pl.ds(0, kk), pl.ds(0, ff)], s.at[slot]
            )
            for w, b, s in ((wg_hbm, wgb, wg_sem), (wu_hbm, wub, wu_sem))
        ]

    def dload(r, e):
        cols = pl.ds(pl.multiple_of(r * 2 * width, width), 2 * width)
        return pltpu.make_async_copy(wd_hbm.at[e, :, cols], wdb.at[e], wd_sem.at[e])

    for e in range(RING):
        go(wload(0, e, e))
    go([dload(0, e) for e in range(experts)])

    barrier = pltpu.get_barrier_semaphore()
    for p in (left, right, partner):
        pl.semaphore_signal(barrier, inc=1, device_id={"ep": p}, device_id_type=MESH)
    me_c[me] = jnp.where(sl[...] < slots, ex[...] * slots + sl[...], -1)
    me_g[me] = ga[...]
    pl.semaphore_wait(barrier, 3)

    def table(i, r, s, dev):
        return [
            rcopy(t.at[s], t.at[s], ms_sem.at[k, i], mr_sem.at[k, r], dev) for k, t in enumerate((me_c, me_g))
        ]

    def tgot(r, s):
        for k, t in enumerate((me_c, me_g)):
            got(t.at[s], mr_sem.at[k, r])

    t_own = table(0, 0, me, right) + table(1, 1, me, left) + table(2, 4, me, partner)
    t_next = table(3, 2, left, right) + table(4, 5, left, partner) + table(5, 6, right, partner)
    t_last = table(6, 7, opp, partner)

    def own(j):
        return [
            rcopy(xall.at[j, me], xall.at[j, me], as_sem.at[0, j], ar_sem.at[0, j], right),
            rcopy(xall.at[j, me], xall.at[j, me], as_sem.at[1, j], ar_sem.at[1, j], left),
            rcopy(xall.at[j, me], xall.at[j, me], as_sem.at[2, j], ar_sem.at[4, j], partner),
        ]

    lo, hi = pl.ds(0, half), pl.ds(half, half)

    def forward(j):
        return [
            rcopy(xall.at[j, left, lo], xall.at[j, left, lo], as_sem.at[3, j], ar_sem.at[2, j], right),
            rcopy(xall.at[j, right, hi], xall.at[j, right, hi], as_sem.at[4, j], ar_sem.at[3, j], left),
            rcopy(xall.at[j, left], xall.at[j, left], as_sem.at[5, j], ar_sem.at[5, j], partner),
            rcopy(xall.at[j, right], xall.at[j, right], as_sem.at[6, j], ar_sem.at[6, j], partner),
        ]

    def across(j):
        return [rcopy(xall.at[j, opp], xall.at[j, opp], as_sem.at[7, j], ar_sem.at[7, j], partner)]

    def send_own(j):
        xload(j).wait()
        go(own(j))

    def step_a(j):
        got(xall.at[j, left], ar_sem.at[0, j])
        got(xall.at[j, right], ar_sem.at[1, j])
        go(forward(j))
        if j + AHEAD < chunks:
            send_own(j + AHEAD)

    def step_b(j):
        got(xall.at[j, opp, lo], ar_sem.at[2, j])
        got(xall.at[j, opp, hi], ar_sem.at[3, j])
        go(across(j))

    def step_c(j):
        for i, s in enumerate(others):
            got(xall.at[j, s], ar_sem.at[4 + i, j])

    A, B, C = (functools.partial(functools.partial, f) for f in (step_a, step_b, step_c))

    go(t_own)
    for j in range(AHEAD):
        send_own(j)
    tgot(0, left)
    tgot(1, right)
    go(t_next)
    tgot(2, opp)
    go(t_last)
    step_a(0)
    for i, s in enumerate(others):
        tgot(4 + i, s)

    def tables(s, _):
        code, g = me_c[s] - rows * me, me_g[s]
        for r0 in range(0, rows, 128):
            size = min(128, rows - r0)
            row = r0 + lax.broadcasted_iota(jnp.int32, (size, tokens), 0)
            w = jnp.zeros((size, tokens), F32)
            d = jnp.zeros((size, tokens), F32)
            for k in range(top):
                hit = row == code[k : k + 1, :]
                w = jnp.where(hit, g[k : k + 1, :], w)
                d = jnp.where(hit, 1.0, d)
            disp[s, r0 : r0 + size, :] = d.astype(BF16)
            comb[s, :, r0 : r0 + size] = w.T.astype(BF16)
        return _

    lax.fori_loop(0, n - 2, tables, 0)
    step_a(1)
    lax.fori_loop(n - 2, n, tables, 0)

    def dispatch(j, k0):
        for q in range(chips):
            a = jnp.dot(disp[2 * q], xall[j, 2 * q], preferred_element_type=F32)
            b = jnp.dot(disp[2 * q + 1], xall[j, 2 * q + 1], preferred_element_type=F32)
            at = slice(q * 2 * slots, (q + 1) * 2 * slots)
            for e in range(experts):
                part = slice(e * slots, (e + 1) * slots)
                z[e, at, k0 : k0 + width] = jnp.concatenate([a[part], b[part]], 0).astype(BF16)

    def gemm1(g, hooks):
        kk = len(GROUPS[g]) * width
        first, last = g == 0, g == len(GROUPS) - 1

        def one(e, _):
            for at, hook in hooks:
                pl.when(e == at)(hook)
            slot = e % RING
            for c in wload(g, e, slot):
                c.wait()
            lhs = z[e, :, :kk]
            for f0 in range(0, ff, width):
                f = slice(f0, f0 + width)
                gg = jnp.dot(lhs, wgb[slot, :kk, f], preferred_element_type=F32)
                uu = jnp.dot(lhs, wub[slot, :kk, f], preferred_element_type=F32)
                if not first:
                    gg += accg[e, :, f]
                    uu += accu[e, :, f]
                if last:
                    h[e, :, f] = (gg * jax.nn.sigmoid(gg) * uu).astype(BF16)
                else:
                    accg[e, :, f] = gg
                    accu[e, :, f] = uu
            pl.when(e + RING < experts)(lambda: go(wload(g, e + RING, slot)))
            if not last:
                pl.when(e + RING >= experts)(lambda: go(wload(g + 1, e + RING - experts, slot)))
            return _

        lax.fori_loop(0, experts, one, 0)

    before = ((B(0), C(0)), (C(1),), (C(2),), (C(3),), (C(4),), (C(5),), (C(6), C(7)))
    within = (
        ((2, A(2)), (5, B(1))),
        ((1, A(3)), (4, B(2))),
        ((1, A(4)), (3, B(3))),
        ((0, A(5)), (2, B(4)), (7, A(6))),
        ((1, B(5)), (6, A(7))),
        ((0, B(6)), (3, B(7))),
        (),
    )
    for g, js in enumerate(GROUPS):
        for f in before[g]:
            f()
        for i, j in enumerate(js):
            dispatch(j, i * width)
        gemm1(g, within[g])

    for c in t_own + t_next + t_last:
        c.wait_send()
    for j in range(chunks):
        for c in own(j) + forward(j) + across(j):
            c.wait_send()

    keep = lambda c, q: accg.at[c, pl.ds(0, tokens), pl.ds(pl.multiple_of(q * width, width), width)]

    def die(c):
        return rcopy(xall.at[c, pl.ds(0, chips)], pr.at[c], ss_sem.at[0, c], sr_sem.at[0, c], partner)

    def far(c):
        return [
            rcopy(xall.at[c, chips, lo], r1.at[c, 0], ss_sem.at[1, c], sr_sem.at[1, c], right),
            rcopy(xall.at[c, chips, hi], r1.at[c, 1], ss_sem.at[2, c], sr_sem.at[2, c], left),
        ]

    def near(c):
        return [
            rcopy(xall.at[c, chips + 1, hi], r2.at[c, 0, hi], ss_sem.at[3, c], sr_sem.at[3, c], right),
            rcopy(xall.at[c, chips + 2, lo], r2.at[c, 1, lo], ss_sem.at[4, c], sr_sem.at[4, c], left),
        ]

    def merged(c):
        return [
            rcopy(xall.at[c, chips + 1, lo], r2.at[c, 0, lo], ss_sem.at[5, c], sr_sem.at[5, c], right),
            rcopy(xall.at[c, chips + 2, hi], r2.at[c, 1, hi], ss_sem.at[6, c], sr_sem.at[6, c], left),
        ]

    def store(c):
        return pltpu.make_async_copy(
            xall.at[c, chips + 3], y_hbm.at[:, pl.ds(pl.multiple_of(c * width, width), width)], y_sem.at[c]
        )

    def both(c, q, at):
        return keep(c, q)[at] + pr[c, q, at].astype(F32)

    def stage1(c):
        die(c).wait_recv()
        xall[c, chips] = both(c, ochip, pl.ds(0, tokens)).astype(BF16)
        xall[c, chips + 1, hi] = both(c, rchip, hi).astype(BF16)
        xall[c, chips + 2, lo] = both(c, lchip, lo).astype(BF16)
        go(far(c) + near(c))

    def stage2(c):
        for k in far(c):
            k.wait_recv()
        xall[c, chips + 1, lo] = (both(c, rchip, lo) + r1[c, 0].astype(F32)).astype(BF16)
        xall[c, chips + 2, hi] = (both(c, lchip, hi) + r1[c, 1].astype(F32)).astype(BF16)
        go(merged(c))

    def stage3(c):
        for k in near(c) + merged(c):
            k.wait_recv()
        total = both(c, chip, pl.ds(0, tokens)) + r2[c, 0].astype(F32) + r2[c, 1].astype(F32)
        xall[c, chips + 3] = total.astype(BF16)
        store(c).start()

    def down(r, k, within, last):
        c = 2 * r + k
        col = slice(k * width, (k + 1) * width)
        for i in range(experts // 2):
            if i % 2 == 0 and k == 0:
                for e in range(2 * i, 2 * i + 4):
                    dload(r, e).wait()
            pieces = [
                jnp.dot(h[e], wdb[e, :, col], preferred_element_type=F32) for e in (2 * i, 2 * i + 1)
            ]
            at = slice(i * 2 * slots, (i + 1) * 2 * slots)
            for s in range(n):
                part = slice(s * slots, (s + 1) * slots)
                z[s, at, :width] = jnp.concatenate([v[part] for v in pieces], 0).astype(BF16)
            if i % 2:
                if k == 1:
                    pl.when(r + 1 < chunks // 2)(lambda: go([dload(r + 1, e) for e in range(2 * i - 2, 2 * i + 2)]))
                (within if i == 1 else last)(c)
        for q in range(chips):
            s = 2 * q + other
            xall[c, q] = jnp.dot(comb[s], z[s, :, :width], preferred_element_type=F32).astype(BF16)
        die(c).start()
        for q in range(chips):
            s = 2 * q + core
            keep(c, q)[...] = jnp.dot(comb[s], z[s, :, :width], preferred_element_type=F32)

    def round_(r, _):
        def within(c):
            pl.when(c >= 1)(lambda: stage1(c - 1))

        def last(c):
            pl.when(c >= 2)(lambda: stage2(c - 2))
            pl.when(c >= 4)(lambda: stage3(c - 4))

        down(r, 0, within, last)
        down(r, 1, within, last)
        return _

    lax.fori_loop(0, chunks // 2, round_, 0)
    c = chunks - 1
    for f, k in ((stage1, 0), (stage2, 1), (stage3, 3), (stage2, 0), (stage3, 2), (stage3, 1), (stage3, 0)):
        f(c - k)

    def drain(c, _):
        die(c).wait_send()
        for k in far(c) + near(c) + merged(c):
            k.wait_send()
        store(c).wait()
        return _

    lax.fori_loop(0, chunks, drain, 0)


def solution(mesh):
    n = mesh.shape["ep"]

    def local(x, expert, slot, gate, w_gate, w_up, w_down):
        tokens, model = x.shape[2:]
        top = expert.shape[3]
        experts, _, ff = w_gate.shape
        slots = 5 * tokens * top // (4 * experts * n)
        rows = experts * slots
        width = 256
        chunks = model // width
        flat = lambda v: v.reshape(tokens, top).T
        vmem = pltpu.VMEM
        dma = pltpu.SemaphoreType.DMA
        any_, inv = pl.BlockSpec(memory_space=pl.ANY), pl.BlockSpec(memory_space=pltpu.VMEM)
        flops = 6 * n * rows * model * ff
        y = pl.pallas_call(
            functools.partial(kernel, n, slots, width),
            out_shape=jax.ShapeDtypeStruct((tokens, model), BF16),
            in_specs=[any_, inv, inv, inv, any_, any_, any_],
            out_specs=any_,
            scratch_shapes=[
                vmem((chunks, n, tokens, width), BF16),
                vmem((experts, n * slots, ff), F32),
                vmem((experts, n * slots, ff), F32),
                vmem((n, rows, 2 * width), BF16),
                vmem((experts, n * slots, ff), BF16),
                vmem((n, rows, tokens), BF16),
                vmem((n, tokens, rows), BF16),
                vmem((RING, 2 * width, ff), BF16),
                vmem((RING, 2 * width, ff), BF16),
                vmem((experts, ff, 2 * width), BF16),
                vmem((n, top, tokens), jnp.int32),
                vmem((n, top, tokens), F32),
                vmem((chunks, n // 2, tokens, width), BF16),
                vmem((chunks, 2, tokens // 2, width), BF16),
                vmem((chunks, 2, tokens, width), BF16),
                dma((chunks,)),
                dma((RING,)),
                dma((RING,)),
                dma((experts,)),
                dma((chunks,)),
                dma((2, 7)),
                dma((2, 8)),
                dma((8, chunks)),
                dma((8, chunks)),
                dma((7, chunks)),
                dma((7, chunks)),
            ],
            compiler_params=pltpu.CompilerParams(
                collective_id=0, has_side_effects=True, vmem_limit_bytes=67_000_000
            ),
            cost_estimate=pl.CostEstimate(
                flops=flops, bytes_accessed=6 * experts * model * ff, transcendentals=n * rows * ff
            ),
            name="moe",
        )(x.reshape(tokens, model), flat(expert), flat(slot), flat(gate), w_gate, w_up, w_down)
        return y.reshape(x.shape)

    token, weight = P("dp", "ep", None, None), P("ep", None, None)
    return jax.shard_map(
        local,
        mesh=mesh,
        in_specs=(token,) * 4 + (weight,) * 3,
        out_specs=token,
        check_vma=False,
    )
```

```python
import functools

import jax
import jax.numpy as jnp
from jax import lax
from jax.experimental import pallas as pl
from jax.experimental.pallas import tpu as pltpu
from jax.sharding import PartitionSpec as P

MESH = pl.DeviceIdType.MESH
F32, BF16 = jnp.float32, jnp.bfloat16
GROUPS = ((0,), (1,), (2,), (3,), (4,), (5,), (6,), (7,))
AHEAD = 2
RING = 4


def kernel(
    n, slots, width,
    x_hbm, ex, sl, ga, wg_hbm, wu_hbm, wd_hbm, y_hbm,
    xall, accg, accu, z, h, disp, comb, wgb, wub, wdb, me_c, me_g, pr, r1, r2,
    x_sem, wg_sem, wu_sem, wd_sem, y_sem, ms_sem, mr_sem, as_sem, ar_sem, ss_sem, sr_sem,
):
    experts = wg_hbm.shape[0]
    tokens = x_hbm.shape[0]
    ff = wg_hbm.shape[2]
    top = ex.shape[0]
    rows = experts * slots
    chunks = xall.shape[0]
    half = tokens // 2
    chips = n // 2
    me = lax.axis_index("ep")
    chip, core = me // 2, me % 2
    other = 1 - core
    lchip, rchip, ochip = (chip + chips - 1) % chips, (chip + 1) % chips, (chip + 2) % chips
    left, right, opp, partner = 2 * lchip + core, 2 * rchip + core, 2 * ochip + core, 2 * chip + other
    others = tuple(2 * q + other for q in (chip, lchip, rchip, ochip))

    def rcopy(src, dst, ssem, rsem, dev):
        return pltpu.make_async_remote_copy(
            src_ref=src, dst_ref=dst, send_sem=ssem, recv_sem=rsem,
            device_id={"ep": dev}, device_id_type=MESH,
        )

    def go(copies):
        for c in copies:
            c.start()

    def got(dst, sem):
        rcopy(dst, dst, sem, sem, partner).wait_recv()

    def xload(j):
        return pltpu.make_async_copy(x_hbm.at[:, pl.ds(j * width, width)], xall.at[j, me], x_sem.at[j])

    go([xload(j) for j in range(chunks)])

    def wload(g, e, slot):
        k0, kk = GROUPS[g][0] * width, len(GROUPS[g]) * width
        return [
            pltpu.make_async_copy(
                w.at[e, pl.ds(k0, kk), :], b.at[slot, pl.ds(0, kk), pl.ds(0, ff)], s.at[slot]
            )
            for w, b, s in ((wg_hbm, wgb, wg_sem), (wu_hbm, wub, wu_sem))
        ]

    def dload(r, e):
        cols = pl.ds(pl.multiple_of(r * 2 * width, width), 2 * width)
        return pltpu.make_async_copy(wd_hbm.at[e, :, cols], wdb.at[e], wd_sem.at[e])

    for e in range(RING):
        go(wload(0, e, e))
    go([dload(0, e) for e in range(experts)])

    barrier = pltpu.get_barrier_semaphore()
    for p in (left, right, partner):
        pl.semaphore_signal(barrier, inc=1, device_id={"ep": p}, device_id_type=MESH)
    me_c[me] = jnp.where(sl[...] < slots, ex[...] * slots + sl[...], -1)
    me_g[me] = ga[...]
    pl.semaphore_wait(barrier, 3)

    def table(i, r, s, dev):
        return [
            rcopy(t.at[s], t.at[s], ms_sem.at[k, i], mr_sem.at[k, r], dev) for k, t in enumerate((me_c, me_g))
        ]

    def tgot(r, s):
        for k, t in enumerate((me_c, me_g)):
            got(t.at[s], mr_sem.at[k, r])

    t_own = table(0, 0, me, right) + table(1, 1, me, left) + table(2, 4, me, partner)
    t_next = table(3, 2, left, right) + table(4, 5, left, partner) + table(5, 6, right, partner)
    t_last = table(6, 7, opp, partner)

    def own(j):
        return [
            rcopy(xall.at[j, me], xall.at[j, me], as_sem.at[0, j], ar_sem.at[0, j], right),
            rcopy(xall.at[j, me], xall.at[j, me], as_sem.at[1, j], ar_sem.at[1, j], left),
            rcopy(xall.at[j, me], xall.at[j, me], as_sem.at[2, j], ar_sem.at[4, j], partner),
        ]

    lo, hi = pl.ds(0, half), pl.ds(half, half)

    def forward(j):
        return [
            rcopy(xall.at[j, left, lo], xall.at[j, left, lo], as_sem.at[3, j], ar_sem.at[2, j], right),
            rcopy(xall.at[j, right, hi], xall.at[j, right, hi], as_sem.at[4, j], ar_sem.at[3, j], left),
            rcopy(xall.at[j, left], xall.at[j, left], as_sem.at[5, j], ar_sem.at[5, j], partner),
            rcopy(xall.at[j, right], xall.at[j, right], as_sem.at[6, j], ar_sem.at[6, j], partner),
        ]

    def across(j):
        return [rcopy(xall.at[j, opp], xall.at[j, opp], as_sem.at[7, j], ar_sem.at[7, j], partner)]

    def send_own(j):
        xload(j).wait()
        go(own(j))

    def step_a(j):
        got(xall.at[j, left], ar_sem.at[0, j])
        got(xall.at[j, right], ar_sem.at[1, j])
        go(forward(j))
        if j + AHEAD < chunks:
            send_own(j + AHEAD)

    def step_b(j):
        got(xall.at[j, opp, lo], ar_sem.at[2, j])
        got(xall.at[j, opp, hi], ar_sem.at[3, j])
        go(across(j))

    def step_c(j):
        for i, s in enumerate(others):
            got(xall.at[j, s], ar_sem.at[4 + i, j])

    A, B = (functools.partial(functools.partial, f) for f in (step_a, step_b))

    go(t_own)
    for j in range(AHEAD):
        send_own(j)
    tgot(0, left)
    tgot(1, right)
    go(t_next)
    tgot(2, opp)
    go(t_last)
    step_a(0)
    for i, s in enumerate(others):
        tgot(4 + i, s)

    def tables(s, _):
        code, g = me_c[s] - rows * me, me_g[s]
        for r0 in range(0, rows, 128):
            size = min(128, rows - r0)
            row = r0 + lax.broadcasted_iota(jnp.int32, (size, tokens), 0)
            w = jnp.zeros((size, tokens), F32)
            d = jnp.zeros((size, tokens), F32)
            for k in range(top):
                hit = row == code[k : k + 1, :]
                w = jnp.where(hit, g[k : k + 1, :], w)
                d = jnp.where(hit, 1.0, d)
            disp[s, r0 : r0 + size, :] = d.astype(BF16)
            comb[s, :, r0 : r0 + size] = w.T.astype(BF16)
        return _

    lax.fori_loop(0, n - 2, tables, 0)
    step_a(1)
    lax.fori_loop(n - 2, n, tables, 0)

    def dispatch(j, k0):
        for q in range(chips):
            a = jnp.dot(disp[2 * q], xall[j, 2 * q], preferred_element_type=F32)
            b = jnp.dot(disp[2 * q + 1], xall[j, 2 * q + 1], preferred_element_type=F32)
            at = slice(q * 2 * slots, (q + 1) * 2 * slots)
            for e in range(experts):
                part = slice(e * slots, (e + 1) * slots)
                z[e, at, k0 : k0 + width] = jnp.concatenate([a[part], b[part]], 0).astype(BF16)

    def gemm1(g, hooks):
        kk = len(GROUPS[g]) * width
        first, last = g == 0, g == len(GROUPS) - 1

        def pair(p, _):
            for at, hook in hooks:
                pl.when(p == at)(hook)
            es = (2 * p, 2 * p + 1)
            for e in es:
                for c in wload(g, e, e % RING):
                    c.wait()
            for e in es:
                lhs = z[e, :, :kk]
                for f0 in range(0, ff, width):
                    f = slice(f0, f0 + width)
                    gg = jnp.dot(lhs, wgb[e % RING, :kk, f], preferred_element_type=F32)
                    uu = jnp.dot(lhs, wub[e % RING, :kk, f], preferred_element_type=F32)
                    if not first:
                        gg += accg[e, :, f]
                        uu += accu[e, :, f]
                    if last:
                        h[e, :, f] = (gg * jax.nn.sigmoid(gg) * uu).astype(BF16)
                    else:
                        accg[e, :, f] = gg
                        accu[e, :, f] = uu
            for e in es:
                pl.when(e + RING < experts)(lambda: go(wload(g, e + RING, e % RING)))
                if not last:
                    pl.when(e + RING >= experts)(lambda: go(wload(g + 1, e + RING - experts, e % RING)))
            return _

        lax.fori_loop(0, experts // 2, pair, 0)

    def within(j):
        return [(at, f(k)) for at, f, k in ((1, A, j + 2), (3, B, j + 1)) if k < chunks]

    for g, js in enumerate(GROUPS):
        for i, j in enumerate(js):
            if j == 0:
                step_b(0)
            step_c(j)
            dispatch(j, i * width)
        gemm1(g, within(js[0]))

    for c in t_own + t_next + t_last:
        c.wait_send()
    for j in range(chunks):
        for c in own(j) + forward(j) + across(j):
            c.wait_send()

    keep = lambda c, q: accg.at[c, pl.ds(0, tokens), pl.ds(pl.multiple_of(q * width, width), width)]

    def die(c):
        return rcopy(xall.at[c, pl.ds(0, chips)], pr.at[c], ss_sem.at[0, c], sr_sem.at[0, c], partner)

    def far(c):
        return [
            rcopy(xall.at[c, chips, lo], r1.at[c, 0], ss_sem.at[1, c], sr_sem.at[1, c], right),
            rcopy(xall.at[c, chips, hi], r1.at[c, 1], ss_sem.at[2, c], sr_sem.at[2, c], left),
        ]

    def near(c):
        return [
            rcopy(xall.at[c, chips + 1, hi], r2.at[c, 0, hi], ss_sem.at[3, c], sr_sem.at[3, c], right),
            rcopy(xall.at[c, chips + 2, lo], r2.at[c, 1, lo], ss_sem.at[4, c], sr_sem.at[4, c], left),
        ]

    def merged(c):
        return [
            rcopy(xall.at[c, chips + 1, lo], r2.at[c, 0, lo], ss_sem.at[5, c], sr_sem.at[5, c], right),
            rcopy(xall.at[c, chips + 2, hi], r2.at[c, 1, hi], ss_sem.at[6, c], sr_sem.at[6, c], left),
        ]

    def store(c):
        return pltpu.make_async_copy(
            xall.at[c, chips + 3], y_hbm.at[:, pl.ds(pl.multiple_of(c * width, width), width)], y_sem.at[c]
        )

    def both(c, q, at):
        return keep(c, q)[at] + pr[c, q, at].astype(F32)

    def stage1(c):
        die(c).wait_recv()
        xall[c, chips] = both(c, ochip, pl.ds(0, tokens)).astype(BF16)
        xall[c, chips + 1, hi] = both(c, rchip, hi).astype(BF16)
        xall[c, chips + 2, lo] = both(c, lchip, lo).astype(BF16)
        go(far(c) + near(c))

    def stage2(c):
        for k in far(c):
            k.wait_recv()
        xall[c, chips + 1, lo] = (both(c, rchip, lo) + r1[c, 0].astype(F32)).astype(BF16)
        xall[c, chips + 2, hi] = (both(c, lchip, hi) + r1[c, 1].astype(F32)).astype(BF16)
        go(merged(c))

    def stage3(c):
        for k in near(c) + merged(c):
            k.wait_recv()
        total = both(c, chip, pl.ds(0, tokens)) + r2[c, 0].astype(F32) + r2[c, 1].astype(F32)
        xall[c, chips + 3] = total.astype(BF16)
        store(c).start()

    def down(r, k, within, last):
        c = 2 * r + k
        col = slice(k * width, (k + 1) * width)
        for i in range(experts // 2):
            if i % 2 == 0 and k == 0:
                for e in range(2 * i, 2 * i + 4):
                    dload(r, e).wait()
            pieces = [
                jnp.dot(h[e], wdb[e, :, col], preferred_element_type=F32) for e in (2 * i, 2 * i + 1)
            ]
            at = slice(i * 2 * slots, (i + 1) * 2 * slots)
            for s in range(n):
                part = slice(s * slots, (s + 1) * slots)
                z[s, at, :width] = jnp.concatenate([v[part] for v in pieces], 0).astype(BF16)
            if i % 2:
                if k == 1:
                    pl.when(r + 1 < chunks // 2)(lambda: go([dload(r + 1, e) for e in range(2 * i - 2, 2 * i + 2)]))
                (within if i == 1 else last)(c)
        for q in range(chips):
            s = 2 * q + other
            xall[c, q] = jnp.dot(comb[s], z[s, :, :width], preferred_element_type=F32).astype(BF16)
        die(c).start()
        for q in range(chips):
            s = 2 * q + core
            keep(c, q)[...] = jnp.dot(comb[s], z[s, :, :width], preferred_element_type=F32)

    def round_(r, _):
        def within(c):
            pl.when(c >= 1)(lambda: stage1(c - 1))

        def last(c):
            pl.when(c >= 2)(lambda: stage2(c - 2))
            pl.when(c >= 4)(lambda: stage3(c - 4))

        down(r, 0, within, last)
        down(r, 1, within, last)
        return _

    lax.fori_loop(0, chunks // 2, round_, 0)
    c = chunks - 1
    for f, k in ((stage1, 0), (stage2, 1), (stage3, 3), (stage2, 0), (stage3, 2), (stage3, 1), (stage3, 0)):
        f(c - k)

    def drain(c, _):
        die(c).wait_send()
        for k in far(c) + near(c) + merged(c):
            k.wait_send()
        store(c).wait()
        return _

    lax.fori_loop(0, chunks, drain, 0)


def solution(mesh):
    n = mesh.shape["ep"]

    def local(x, expert, slot, gate, w_gate, w_up, w_down):
        tokens, model = x.shape[2:]
        top = expert.shape[3]
        experts, _, ff = w_gate.shape
        slots = 5 * tokens * top // (4 * experts * n)
        rows = experts * slots
        width = 256
        chunks = model // width
        flat = lambda v: v.reshape(tokens, top).T
        vmem = pltpu.VMEM
        dma = pltpu.SemaphoreType.DMA
        any_, inv = pl.BlockSpec(memory_space=pl.ANY), pl.BlockSpec(memory_space=pltpu.VMEM)
        flops = 6 * n * rows * model * ff
        y = pl.pallas_call(
            functools.partial(kernel, n, slots, width),
            out_shape=jax.ShapeDtypeStruct((tokens, model), BF16),
            in_specs=[any_, inv, inv, inv, any_, any_, any_],
            out_specs=any_,
            scratch_shapes=[
                vmem((chunks, n, tokens, width), BF16),
                vmem((experts, n * slots, ff), F32),
                vmem((experts, n * slots, ff), F32),
                vmem((n, rows, width), BF16),
                vmem((experts, n * slots, ff), BF16),
                vmem((n, rows, tokens), BF16),
                vmem((n, tokens, rows), BF16),
                vmem((RING, width, ff), BF16),
                vmem((RING, width, ff), BF16),
                vmem((experts, ff, 2 * width), BF16),
                vmem((n, top, tokens), jnp.int32),
                vmem((n, top, tokens), F32),
                vmem((chunks, n // 2, tokens, width), BF16),
                vmem((chunks, 2, tokens // 2, width), BF16),
                vmem((chunks, 2, tokens, width), BF16),
                dma((chunks,)),
                dma((RING,)),
                dma((RING,)),
                dma((experts,)),
                dma((chunks,)),
                dma((2, 7)),
                dma((2, 8)),
                dma((8, chunks)),
                dma((8, chunks)),
                dma((7, chunks)),
                dma((7, chunks)),
            ],
            compiler_params=pltpu.CompilerParams(
                collective_id=0, has_side_effects=True, vmem_limit_bytes=67_000_000
            ),
            cost_estimate=pl.CostEstimate(
                flops=flops, bytes_accessed=6 * experts * model * ff, transcendentals=n * rows * ff
            ),
            name="moe",
        )(x.reshape(tokens, model), flat(expert), flat(slot), flat(gate), w_gate, w_up, w_down)
        return y.reshape(x.shape)

    token, weight = P("dp", "ep", None, None), P("ep", None, None)
    return jax.shard_map(
        local,
        mesh=mesh,
        in_specs=(token,) * 4 + (weight,) * 3,
        out_specs=token,
        check_vma=False,
    )
```

```python
import functools

import jax
import jax.numpy as jnp
from jax import lax
from jax.experimental import pallas as pl
from jax.experimental.pallas import tpu as pltpu
from jax.sharding import PartitionSpec as P

MESH = pl.DeviceIdType.MESH
F32, BF16 = jnp.float32, jnp.bfloat16
GROUPS = ((0,), (1,), (2,), (3,), (4,), (5,), (6,), (7,))
AHEAD = 2
RING = 4


def kernel(
    n, slots, width,
    x_hbm, ex, sl, ga, wg_hbm, wu_hbm, wd_hbm, y_hbm,
    xall, accg, accu, z, h, disp, comb, wgb, wub, wdb, me_c, me_g, pr, r1, r2,
    x_sem, wg_sem, wu_sem, wd_sem, y_sem, ms_sem, mr_sem, as_sem, ar_sem, ss_sem, sr_sem,
):
    experts = wg_hbm.shape[0]
    tokens = x_hbm.shape[0]
    ff = wg_hbm.shape[2]
    top = ex.shape[0]
    rows = experts * slots
    chunks = xall.shape[0]
    half = tokens // 2
    chips = n // 2
    me = lax.axis_index("ep")
    chip, core = me // 2, me % 2
    other = 1 - core
    lchip, rchip, ochip = (chip + chips - 1) % chips, (chip + 1) % chips, (chip + 2) % chips
    left, right, opp, partner = 2 * lchip + core, 2 * rchip + core, 2 * ochip + core, 2 * chip + other
    others = tuple(2 * q + other for q in (chip, lchip, rchip, ochip))

    def rcopy(src, dst, ssem, rsem, dev):
        return pltpu.make_async_remote_copy(
            src_ref=src, dst_ref=dst, send_sem=ssem, recv_sem=rsem,
            device_id={"ep": dev}, device_id_type=MESH,
        )

    def go(copies):
        for c in copies:
            c.start()

    def got(dst, sem):
        rcopy(dst, dst, sem, sem, partner).wait_recv()

    def xload(j):
        return pltpu.make_async_copy(x_hbm.at[:, pl.ds(j * width, width)], xall.at[j, me], x_sem.at[j])

    go([xload(j) for j in range(chunks)])

    def wload(g, e, slot):
        k0, kk = GROUPS[g][0] * width, len(GROUPS[g]) * width
        return [
            pltpu.make_async_copy(
                w.at[e, pl.ds(k0, kk), :], b.at[slot, pl.ds(0, kk), pl.ds(0, ff)], s.at[slot]
            )
            for w, b, s in ((wg_hbm, wgb, wg_sem), (wu_hbm, wub, wu_sem))
        ]

    def dload(r, e):
        cols = pl.ds(pl.multiple_of(r * 2 * width, width), 2 * width)
        return pltpu.make_async_copy(wd_hbm.at[e, :, cols], wdb.at[e], wd_sem.at[e])

    for e in range(RING):
        go(wload(0, e, e))
    go([dload(0, e) for e in range(experts)])

    barrier = pltpu.get_barrier_semaphore()
    for p in (left, right, partner):
        pl.semaphore_signal(barrier, inc=1, device_id={"ep": p}, device_id_type=MESH)
    me_c[me] = jnp.where(sl[...] < slots, ex[...] * slots + sl[...], -1)
    me_g[me] = ga[...]
    pl.semaphore_wait(barrier, 3)

    def table(i, r, s, dev):
        return [
            rcopy(t.at[s], t.at[s], ms_sem.at[k, i], mr_sem.at[k, r], dev) for k, t in enumerate((me_c, me_g))
        ]

    def tgot(r, s):
        for k, t in enumerate((me_c, me_g)):
            got(t.at[s], mr_sem.at[k, r])

    t_own = table(0, 0, me, right) + table(1, 1, me, left) + table(2, 4, me, partner)
    t_next = table(3, 2, left, right) + table(4, 5, left, partner) + table(5, 6, right, partner)
    t_last = table(6, 7, opp, partner)

    def own(j):
        return [
            rcopy(xall.at[j, me], xall.at[j, me], as_sem.at[0, j], ar_sem.at[0, j], right),
            rcopy(xall.at[j, me], xall.at[j, me], as_sem.at[1, j], ar_sem.at[1, j], left),
            rcopy(xall.at[j, me], xall.at[j, me], as_sem.at[2, j], ar_sem.at[4, j], partner),
        ]

    lo, hi = pl.ds(0, half), pl.ds(half, half)

    def forward(j):
        return [
            rcopy(xall.at[j, left, lo], xall.at[j, left, lo], as_sem.at[3, j], ar_sem.at[2, j], right),
            rcopy(xall.at[j, right, hi], xall.at[j, right, hi], as_sem.at[4, j], ar_sem.at[3, j], left),
            rcopy(xall.at[j, left], xall.at[j, left], as_sem.at[5, j], ar_sem.at[5, j], partner),
            rcopy(xall.at[j, right], xall.at[j, right], as_sem.at[6, j], ar_sem.at[6, j], partner),
        ]

    def across(j):
        return [rcopy(xall.at[j, opp], xall.at[j, opp], as_sem.at[7, j], ar_sem.at[7, j], partner)]

    def send_own(j):
        xload(j).wait()
        go(own(j))

    def step_a(j):
        got(xall.at[j, left], ar_sem.at[0, j])
        got(xall.at[j, right], ar_sem.at[1, j])
        go(forward(j))
        if j + AHEAD < chunks:
            send_own(j + AHEAD)

    def step_b(j):
        got(xall.at[j, opp, lo], ar_sem.at[2, j])
        got(xall.at[j, opp, hi], ar_sem.at[3, j])
        go(across(j))

    def step_c(j):
        for i, s in enumerate(others):
            got(xall.at[j, s], ar_sem.at[4 + i, j])

    A, B = (functools.partial(functools.partial, f) for f in (step_a, step_b))

    go(t_own)
    for j in range(AHEAD):
        send_own(j)
    tgot(0, left)
    tgot(1, right)
    go(t_next)
    tgot(2, opp)
    go(t_last)
    step_a(0)
    for i, s in enumerate(others):
        tgot(4 + i, s)

    def tables(s, _):
        code, g = me_c[s] - rows * me, me_g[s]
        for r0 in range(0, rows, 128):
            size = min(128, rows - r0)
            row = r0 + lax.broadcasted_iota(jnp.int32, (size, tokens), 0)
            w = jnp.zeros((size, tokens), F32)
            d = jnp.zeros((size, tokens), F32)
            for k in range(top):
                hit = row == code[k : k + 1, :]
                w = jnp.where(hit, g[k : k + 1, :], w)
                d = jnp.where(hit, 1.0, d)
            disp[s, r0 : r0 + size, :] = d.astype(BF16)
            comb[s, :, r0 : r0 + size] = w.T.astype(BF16)
        return _

    lax.fori_loop(0, n - 2, tables, 0)
    step_a(1)
    lax.fori_loop(n - 2, n, tables, 0)

    def dispatch(j, k0):
        for q in range(chips):
            a = jnp.dot(disp[2 * q], xall[j, 2 * q], preferred_element_type=F32)
            b = jnp.dot(disp[2 * q + 1], xall[j, 2 * q + 1], preferred_element_type=F32)
            at = slice(q * 2 * slots, (q + 1) * 2 * slots)
            for e in range(experts):
                part = slice(e * slots, (e + 1) * slots)
                z[e, at, k0 : k0 + width] = jnp.concatenate([a[part], b[part]], 0).astype(BF16)

    def gemm1(g, hooks):
        kk = len(GROUPS[g]) * width
        first, last = g == 0, g == len(GROUPS) - 1

        def pair(p, _):
            for at, hook in hooks:
                pl.when(p == at)(hook)
            es = (2 * p, 2 * p + 1)
            for e in es:
                for c in wload(g, e, e % RING):
                    c.wait()
            for e in es:
                lhs = z[e, :, :kk]
                for f0 in range(0, ff, width):
                    f = slice(f0, f0 + width)
                    gg = jnp.dot(lhs, wgb[e % RING, :kk, f], preferred_element_type=F32)
                    uu = jnp.dot(lhs, wub[e % RING, :kk, f], preferred_element_type=F32)
                    if not first:
                        gg += accg[e, :, f]
                        uu += accu[e, :, f]
                    if last:
                        h[e, :, f] = (gg * jax.nn.sigmoid(gg) * uu).astype(BF16)
                    else:
                        accg[e, :, f] = gg
                        accu[e, :, f] = uu
            for e in es:
                pl.when(e + RING < experts)(lambda: go(wload(g, e + RING, e % RING)))
                if not last:
                    pl.when(e + RING >= experts)(lambda: go(wload(g + 1, e + RING - experts, e % RING)))
            return _

        lax.fori_loop(0, experts // 2, pair, 0)

    def within(j):
        return [(at, f(k)) for at, f, k in ((1, A, j + 2), (2, B, j + 1)) if k < chunks]

    for g, js in enumerate(GROUPS):
        for i, j in enumerate(js):
            if j == 0:
                step_b(0)
            step_c(j)
            dispatch(j, i * width)
        gemm1(g, within(js[0]))

    for c in t_own + t_next + t_last:
        c.wait_send()
    for j in range(chunks):
        for c in own(j) + forward(j) + across(j):
            c.wait_send()

    keep = lambda c, q: accg.at[c, pl.ds(0, tokens), pl.ds(pl.multiple_of(q * width, width), width)]

    def die(c):
        return rcopy(xall.at[c, pl.ds(0, chips)], pr.at[c], ss_sem.at[0, c], sr_sem.at[0, c], partner)

    def far(c):
        return [
            rcopy(xall.at[c, chips, lo], r1.at[c, 0], ss_sem.at[1, c], sr_sem.at[1, c], right),
            rcopy(xall.at[c, chips, hi], r1.at[c, 1], ss_sem.at[2, c], sr_sem.at[2, c], left),
        ]

    def near(c):
        return [
            rcopy(xall.at[c, chips + 1, hi], r2.at[c, 0, hi], ss_sem.at[3, c], sr_sem.at[3, c], right),
            rcopy(xall.at[c, chips + 2, lo], r2.at[c, 1, lo], ss_sem.at[4, c], sr_sem.at[4, c], left),
        ]

    def merged(c):
        return [
            rcopy(xall.at[c, chips + 1, lo], r2.at[c, 0, lo], ss_sem.at[5, c], sr_sem.at[5, c], right),
            rcopy(xall.at[c, chips + 2, hi], r2.at[c, 1, hi], ss_sem.at[6, c], sr_sem.at[6, c], left),
        ]

    def store(c):
        return pltpu.make_async_copy(
            xall.at[c, chips + 3], y_hbm.at[:, pl.ds(pl.multiple_of(c * width, width), width)], y_sem.at[c]
        )

    def both(c, q, at):
        return keep(c, q)[at] + pr[c, q, at].astype(F32)

    def stage1(c):
        die(c).wait_recv()
        xall[c, chips] = both(c, ochip, pl.ds(0, tokens)).astype(BF16)
        xall[c, chips + 1, hi] = both(c, rchip, hi).astype(BF16)
        xall[c, chips + 2, lo] = both(c, lchip, lo).astype(BF16)
        go(far(c) + near(c))

    def stage2(c):
        for k in far(c):
            k.wait_recv()
        xall[c, chips + 1, lo] = (both(c, rchip, lo) + r1[c, 0].astype(F32)).astype(BF16)
        xall[c, chips + 2, hi] = (both(c, lchip, hi) + r1[c, 1].astype(F32)).astype(BF16)
        go(merged(c))

    def stage3(c):
        for k in near(c) + merged(c):
            k.wait_recv()
        total = both(c, chip, pl.ds(0, tokens)) + r2[c, 0].astype(F32) + r2[c, 1].astype(F32)
        xall[c, chips + 3] = total.astype(BF16)
        store(c).start()

    def down(r, k, within, last):
        c = 2 * r + k
        col = slice(k * width, (k + 1) * width)
        for i in range(experts // 2):
            if i % 2 == 0 and k == 0:
                for e in range(2 * i, 2 * i + 4):
                    dload(r, e).wait()
            pieces = [
                jnp.dot(h[e], wdb[e, :, col], preferred_element_type=F32) for e in (2 * i, 2 * i + 1)
            ]
            at = slice(i * 2 * slots, (i + 1) * 2 * slots)
            for s in range(n):
                part = slice(s * slots, (s + 1) * slots)
                z[s, at, :width] = jnp.concatenate([v[part] for v in pieces], 0).astype(BF16)
            if i % 2:
                if k == 1:
                    pl.when(r + 1 < chunks // 2)(lambda: go([dload(r + 1, e) for e in range(2 * i - 2, 2 * i + 2)]))
                (within if i == 1 else last)(c)
        for q in range(chips):
            s = 2 * q + other
            xall[c, q] = jnp.dot(comb[s], z[s, :, :width], preferred_element_type=F32).astype(BF16)
        die(c).start()
        for q in range(chips):
            s = 2 * q + core
            keep(c, q)[...] = jnp.dot(comb[s], z[s, :, :width], preferred_element_type=F32)

    def round_(r, _):
        def within(c):
            pl.when(c >= 1)(lambda: stage1(c - 1))

        def last(c):
            pl.when(c >= 2)(lambda: stage2(c - 2))
            pl.when(c >= 4)(lambda: stage3(c - 4))

        down(r, 0, within, last)
        down(r, 1, within, last)
        return _

    lax.fori_loop(0, chunks // 2, round_, 0)
    c = chunks - 1
    for f, k in ((stage1, 0), (stage2, 1), (stage3, 3), (stage2, 0), (stage3, 2), (stage3, 1), (stage3, 0)):
        f(c - k)

    def drain(c, _):
        die(c).wait_send()
        for k in far(c) + near(c) + merged(c):
            k.wait_send()
        store(c).wait()
        return _

    lax.fori_loop(0, chunks, drain, 0)


def solution(mesh):
    n = mesh.shape["ep"]

    def local(x, expert, slot, gate, w_gate, w_up, w_down):
        tokens, model = x.shape[2:]
        top = expert.shape[3]
        experts, _, ff = w_gate.shape
        slots = 5 * tokens * top // (4 * experts * n)
        rows = experts * slots
        width = 256
        chunks = model // width
        flat = lambda v: v.reshape(tokens, top).T
        vmem = pltpu.VMEM
        dma = pltpu.SemaphoreType.DMA
        any_, inv = pl.BlockSpec(memory_space=pl.ANY), pl.BlockSpec(memory_space=pltpu.VMEM)
        flops = 6 * n * rows * model * ff
        y = pl.pallas_call(
            functools.partial(kernel, n, slots, width),
            out_shape=jax.ShapeDtypeStruct((tokens, model), BF16),
            in_specs=[any_, inv, inv, inv, any_, any_, any_],
            out_specs=any_,
            scratch_shapes=[
                vmem((chunks, n, tokens, width), BF16),
                vmem((experts, n * slots, ff), F32),
                vmem((experts, n * slots, ff), F32),
                vmem((n, rows, width), BF16),
                vmem((experts, n * slots, ff), BF16),
                vmem((n, rows, tokens), BF16),
                vmem((n, tokens, rows), BF16),
                vmem((RING, width, ff), BF16),
                vmem((RING, width, ff), BF16),
                vmem((experts, ff, 2 * width), BF16),
                vmem((n, top, tokens), jnp.int32),
                vmem((n, top, tokens), F32),
                vmem((chunks, n // 2, tokens, width), BF16),
                vmem((chunks, 2, tokens // 2, width), BF16),
                vmem((chunks, 2, tokens, width), BF16),
                dma((chunks,)),
                dma((RING,)),
                dma((RING,)),
                dma((experts,)),
                dma((chunks,)),
                dma((2, 7)),
                dma((2, 8)),
                dma((8, chunks)),
                dma((8, chunks)),
                dma((7, chunks)),
                dma((7, chunks)),
            ],
            compiler_params=pltpu.CompilerParams(
                collective_id=0, has_side_effects=True, vmem_limit_bytes=67_000_000
            ),
            cost_estimate=pl.CostEstimate(
                flops=flops, bytes_accessed=6 * experts * model * ff, transcendentals=n * rows * ff
            ),
            name="moe",
        )(x.reshape(tokens, model), flat(expert), flat(slot), flat(gate), w_gate, w_up, w_down)
        return y.reshape(x.shape)

    token, weight = P("dp", "ep", None, None), P("ep", None, None)
    return jax.shard_map(
        local,
        mesh=mesh,
        in_specs=(token,) * 4 + (weight,) * 3,
        out_specs=token,
        check_vma=False,
    )
```

```python
import functools

import jax
import jax.numpy as jnp
from jax import lax
from jax.experimental import pallas as pl
from jax.experimental.pallas import tpu as pltpu
from jax.sharding import PartitionSpec as P

MESH = pl.DeviceIdType.MESH
F32, BF16 = jnp.float32, jnp.bfloat16
GROUPS = ((0,), (1,), (2,), (3,), (4,), (5,), (6,), (7,))
AHEAD = 2


def kernel(
    n, slots, width,
    x_hbm, ex, sl, ga, wg_hbm, wu_hbm, wd_hbm, y_hbm,
    xall, accg, accu, z, h, disp, comb, wgb, wub, wdb, me_c, me_g, pr, r1, r2,
    x_sem, wg_sem, wu_sem, wd_sem, y_sem, ms_sem, mr_sem, as_sem, ar_sem, ss_sem, sr_sem,
):
    experts = wg_hbm.shape[0]
    tokens = x_hbm.shape[0]
    ff = wg_hbm.shape[2]
    top = ex.shape[0]
    rows = experts * slots
    chunks = xall.shape[0]
    half = tokens // 2
    chips = n // 2
    me = lax.axis_index("ep")
    chip, core = me // 2, me % 2
    other = 1 - core
    lchip, rchip, ochip = (chip + chips - 1) % chips, (chip + 1) % chips, (chip + 2) % chips
    left, right, opp, partner = 2 * lchip + core, 2 * rchip + core, 2 * ochip + core, 2 * chip + other
    others = tuple(2 * q + other for q in (chip, lchip, rchip, ochip))

    def rcopy(src, dst, ssem, rsem, dev):
        return pltpu.make_async_remote_copy(
            src_ref=src, dst_ref=dst, send_sem=ssem, recv_sem=rsem,
            device_id={"ep": dev}, device_id_type=MESH,
        )

    def go(copies):
        for c in copies:
            c.start()

    def got(dst, sem):
        rcopy(dst, dst, sem, sem, partner).wait_recv()

    def xload(j):
        return pltpu.make_async_copy(x_hbm.at[:, pl.ds(j * width, width)], xall.at[j, me], x_sem.at[j])

    go([xload(j) for j in range(chunks)])

    def wload(g, e):
        k0, kk = GROUPS[g][0] * width, len(GROUPS[g]) * width
        return [
            pltpu.make_async_copy(
                w.at[e, pl.ds(k0, kk), :], b.at[e, pl.ds(0, kk), :], s.at[e]
            )
            for w, b, s in ((wg_hbm, wgb, wg_sem), (wu_hbm, wub, wu_sem))
        ]

    def dload(r, e):
        cols = pl.ds(pl.multiple_of(r * 2 * width, width), 2 * width)
        return pltpu.make_async_copy(wd_hbm.at[e, :, cols], wdb.at[e], wd_sem.at[e])

    for e in range(experts):
        go(wload(0, e))
    go([dload(0, e) for e in range(experts)])

    barrier = pltpu.get_barrier_semaphore()
    for p in (left, right, partner):
        pl.semaphore_signal(barrier, inc=1, device_id={"ep": p}, device_id_type=MESH)
    me_c[me] = jnp.where(sl[...] < slots, ex[...] * slots + sl[...], -1)
    me_g[me] = ga[...]
    pl.semaphore_wait(barrier, 3)

    def table(i, r, s, dev):
        return [
            rcopy(t.at[s], t.at[s], ms_sem.at[k, i], mr_sem.at[k, r], dev) for k, t in enumerate((me_c, me_g))
        ]

    def tgot(r, s):
        for k, t in enumerate((me_c, me_g)):
            got(t.at[s], mr_sem.at[k, r])

    t_own = table(0, 0, me, right) + table(1, 1, me, left) + table(2, 4, me, partner)
    t_next = table(3, 2, left, right) + table(4, 5, left, partner) + table(5, 6, right, partner)
    t_last = table(6, 7, opp, partner)

    def own(j):
        return [
            rcopy(xall.at[j, me], xall.at[j, me], as_sem.at[0, j], ar_sem.at[0, j], right),
            rcopy(xall.at[j, me], xall.at[j, me], as_sem.at[1, j], ar_sem.at[1, j], left),
            rcopy(xall.at[j, me], xall.at[j, me], as_sem.at[2, j], ar_sem.at[4, j], partner),
        ]

    lo, hi = pl.ds(0, half), pl.ds(half, half)

    def forward(j):
        return [
            rcopy(xall.at[j, left, lo], xall.at[j, left, lo], as_sem.at[3, j], ar_sem.at[2, j], right),
            rcopy(xall.at[j, right, hi], xall.at[j, right, hi], as_sem.at[4, j], ar_sem.at[3, j], left),
            rcopy(xall.at[j, left], xall.at[j, left], as_sem.at[5, j], ar_sem.at[5, j], partner),
            rcopy(xall.at[j, right], xall.at[j, right], as_sem.at[6, j], ar_sem.at[6, j], partner),
        ]

    def across(j):
        return [rcopy(xall.at[j, opp], xall.at[j, opp], as_sem.at[7, j], ar_sem.at[7, j], partner)]

    def send_own(j):
        xload(j).wait()
        go(own(j))

    def step_a(j):
        got(xall.at[j, left], ar_sem.at[0, j])
        got(xall.at[j, right], ar_sem.at[1, j])
        go(forward(j))
        if j + AHEAD < chunks:
            send_own(j + AHEAD)

    def step_b(j):
        got(xall.at[j, opp, lo], ar_sem.at[2, j])
        got(xall.at[j, opp, hi], ar_sem.at[3, j])
        go(across(j))

    def step_c(j):
        for i, s in enumerate(others):
            got(xall.at[j, s], ar_sem.at[4 + i, j])

    A, B = (functools.partial(functools.partial, f) for f in (step_a, step_b))

    go(t_own)
    for j in range(AHEAD):
        send_own(j)
    tgot(0, left)
    tgot(1, right)
    go(t_next)
    tgot(2, opp)
    go(t_last)
    step_a(0)
    for i, s in enumerate(others):
        tgot(4 + i, s)

    def tables(s, _):
        code, g = me_c[s] - rows * me, me_g[s]
        for r0 in range(0, rows, 128):
            size = min(128, rows - r0)
            row = r0 + lax.broadcasted_iota(jnp.int32, (size, tokens), 0)
            w = jnp.zeros((size, tokens), F32)
            d = jnp.zeros((size, tokens), F32)
            for k in range(top):
                hit = row == code[k : k + 1, :]
                w = jnp.where(hit, g[k : k + 1, :], w)
                d = jnp.where(hit, 1.0, d)
            disp[s, r0 : r0 + size, :] = d.astype(BF16)
            comb[s, :, r0 : r0 + size] = w.T.astype(BF16)
        return _

    lax.fori_loop(0, n - 2, tables, 0)
    step_a(1)
    lax.fori_loop(n - 2, n, tables, 0)

    def dispatch(j, k0):
        for q in range(chips):
            a = jnp.dot(disp[2 * q], xall[j, 2 * q], preferred_element_type=F32)
            b = jnp.dot(disp[2 * q + 1], xall[j, 2 * q + 1], preferred_element_type=F32)
            at = slice(q * 2 * slots, (q + 1) * 2 * slots)
            for e in range(experts):
                part = slice(e * slots, (e + 1) * slots)
                z[e, at, k0 : k0 + width] = jnp.concatenate([a[part], b[part]], 0).astype(BF16)

    def gemm1(g, hooks):
        kk = len(GROUPS[g]) * width
        first, last = g == 0, g == len(GROUPS) - 1

        def pair(p, _):
            for at, hook in hooks:
                pl.when(p == at)(hook)
            es = (2 * p, 2 * p + 1)
            for e in es:
                for c in wload(g, e):
                    c.wait()
            for e in es:
                lhs = z[e, :, :kk]
                for f0 in range(0, ff, width):
                    f = slice(f0, f0 + width)
                    gg = jnp.dot(lhs, wgb[e, :kk, f], preferred_element_type=F32)
                    uu = jnp.dot(lhs, wub[e, :kk, f], preferred_element_type=F32)
                    if not first:
                        gg += accg[e, :, f]
                        uu += accu[e, :, f]
                    if last:
                        h[e, :, f] = (gg * jax.nn.sigmoid(gg) * uu).astype(BF16)
                    else:
                        accg[e, :, f] = gg
                        accu[e, :, f] = uu
            if not last:
                for e in es:
                    go(wload(g + 1, e))
            return _

        lax.fori_loop(0, experts // 2, pair, 0)

    def within(j):
        return [(at, f(k)) for at, f, k in ((1, A, j + 2), (2, B, j + 1)) if k < chunks]

    for g, js in enumerate(GROUPS):
        for i, j in enumerate(js):
            if j == 0:
                step_b(0)
            step_c(j)
            dispatch(j, i * width)
        gemm1(g, within(js[0]))

    for c in t_own + t_next + t_last:
        c.wait_send()
    for j in range(chunks):
        for c in own(j) + forward(j) + across(j):
            c.wait_send()

    keep = lambda c, q: accg.at[c, pl.ds(0, tokens), pl.ds(pl.multiple_of(q * width, width), width)]

    def die(c):
        return rcopy(xall.at[c, pl.ds(0, chips)], pr.at[c], ss_sem.at[0, c], sr_sem.at[0, c], partner)

    def far(c):
        return [
            rcopy(xall.at[c, chips, lo], r1.at[c, 0], ss_sem.at[1, c], sr_sem.at[1, c], right),
            rcopy(xall.at[c, chips, hi], r1.at[c, 1], ss_sem.at[2, c], sr_sem.at[2, c], left),
        ]

    def near(c):
        return [
            rcopy(xall.at[c, chips + 1, hi], r2.at[c, 0, hi], ss_sem.at[3, c], sr_sem.at[3, c], right),
            rcopy(xall.at[c, chips + 2, lo], r2.at[c, 1, lo], ss_sem.at[4, c], sr_sem.at[4, c], left),
        ]

    def merged(c):
        return [
            rcopy(xall.at[c, chips + 1, lo], r2.at[c, 0, lo], ss_sem.at[5, c], sr_sem.at[5, c], right),
            rcopy(xall.at[c, chips + 2, hi], r2.at[c, 1, hi], ss_sem.at[6, c], sr_sem.at[6, c], left),
        ]

    def store(c):
        return pltpu.make_async_copy(
            xall.at[c, chips + 3], y_hbm.at[:, pl.ds(pl.multiple_of(c * width, width), width)], y_sem.at[c]
        )

    def both(c, q, at):
        return keep(c, q)[at] + pr[c, q, at].astype(F32)

    def stage1(c):
        die(c).wait_recv()
        xall[c, chips] = both(c, ochip, pl.ds(0, tokens)).astype(BF16)
        xall[c, chips + 1, hi] = both(c, rchip, hi).astype(BF16)
        xall[c, chips + 2, lo] = both(c, lchip, lo).astype(BF16)
        go(far(c) + near(c))

    def stage2(c):
        for k in far(c):
            k.wait_recv()
        xall[c, chips + 1, lo] = (both(c, rchip, lo) + r1[c, 0].astype(F32)).astype(BF16)
        xall[c, chips + 2, hi] = (both(c, lchip, hi) + r1[c, 1].astype(F32)).astype(BF16)
        go(merged(c))

    def stage3(c):
        for k in near(c) + merged(c):
            k.wait_recv()
        total = both(c, chip, pl.ds(0, tokens)) + r2[c, 0].astype(F32) + r2[c, 1].astype(F32)
        xall[c, chips + 3] = total.astype(BF16)
        store(c).start()

    def down(r, k, within, last):
        c = 2 * r + k
        col = slice(k * width, (k + 1) * width)
        for i in range(experts // 2):
            if i % 2 == 0 and k == 0:
                for e in range(2 * i, 2 * i + 4):
                    dload(r, e).wait()
            pieces = [
                jnp.dot(h[e], wdb[e, :, col], preferred_element_type=F32) for e in (2 * i, 2 * i + 1)
            ]
            at = slice(i * 2 * slots, (i + 1) * 2 * slots)
            for s in range(n):
                part = slice(s * slots, (s + 1) * slots)
                z[s, at, :width] = jnp.concatenate([v[part] for v in pieces], 0).astype(BF16)
            if i % 2:
                if k == 1:
                    pl.when(r + 1 < chunks // 2)(lambda: go([dload(r + 1, e) for e in range(2 * i - 2, 2 * i + 2)]))
                (within if i == 1 else last)(c)
        for q in range(chips):
            s = 2 * q + other
            xall[c, q] = jnp.dot(comb[s], z[s, :, :width], preferred_element_type=F32).astype(BF16)
        die(c).start()
        for q in range(chips):
            s = 2 * q + core
            keep(c, q)[...] = jnp.dot(comb[s], z[s, :, :width], preferred_element_type=F32)

    def round_(r, _):
        def within(c):
            pl.when(c >= 1)(lambda: stage1(c - 1))

        def last(c):
            pl.when(c >= 2)(lambda: stage2(c - 2))
            pl.when(c >= 4)(lambda: stage3(c - 4))

        down(r, 0, within, last)
        down(r, 1, within, last)
        return _

    lax.fori_loop(0, chunks // 2, round_, 0)
    c = chunks - 1
    for f, k in ((stage1, 0), (stage2, 1), (stage3, 3), (stage2, 0), (stage3, 2), (stage3, 1), (stage3, 0)):
        f(c - k)

    def drain(c, _):
        die(c).wait_send()
        for k in far(c) + near(c) + merged(c):
            k.wait_send()
        store(c).wait()
        return _

    lax.fori_loop(0, chunks, drain, 0)


def solution(mesh):
    n = mesh.shape["ep"]

    def local(x, expert, slot, gate, w_gate, w_up, w_down):
        tokens, model = x.shape[2:]
        top = expert.shape[3]
        experts, _, ff = w_gate.shape
        slots = 5 * tokens * top // (4 * experts * n)
        rows = experts * slots
        width = 256
        chunks = model // width
        flat = lambda v: v.reshape(tokens, top).T
        vmem = pltpu.VMEM
        dma = pltpu.SemaphoreType.DMA
        any_, inv = pl.BlockSpec(memory_space=pl.ANY), pl.BlockSpec(memory_space=pltpu.VMEM)
        flops = 6 * n * rows * model * ff
        y = pl.pallas_call(
            functools.partial(kernel, n, slots, width),
            out_shape=jax.ShapeDtypeStruct((tokens, model), BF16),
            in_specs=[any_, inv, inv, inv, any_, any_, any_],
            out_specs=any_,
            scratch_shapes=[
                vmem((chunks, n, tokens, width), BF16),
                vmem((experts, n * slots, ff), F32),
                vmem((experts, n * slots, ff), F32),
                vmem((n, rows, width), BF16),
                vmem((experts, n * slots, ff), BF16),
                vmem((n, rows, tokens), BF16),
                vmem((n, tokens, rows), BF16),
                vmem((experts, width, ff), BF16),
                vmem((experts, width, ff), BF16),
                vmem((experts, ff, 2 * width), BF16),
                vmem((n, top, tokens), jnp.int32),
                vmem((n, top, tokens), F32),
                vmem((chunks, n // 2, tokens, width), BF16),
                vmem((chunks, 2, tokens // 2, width), BF16),
                vmem((chunks, 2, tokens, width), BF16),
                dma((chunks,)),
                dma((experts,)),
                dma((experts,)),
                dma((experts,)),
                dma((chunks,)),
                dma((2, 7)),
                dma((2, 8)),
                dma((8, chunks)),
                dma((8, chunks)),
                dma((7, chunks)),
                dma((7, chunks)),
            ],
            compiler_params=pltpu.CompilerParams(
                collective_id=0, has_side_effects=True, vmem_limit_bytes=67_000_000
            ),
            cost_estimate=pl.CostEstimate(
                flops=flops, bytes_accessed=6 * experts * model * ff, transcendentals=n * rows * ff
            ),
            name="moe",
        )(x.reshape(tokens, model), flat(expert), flat(slot), flat(gate), w_gate, w_up, w_down)
        return y.reshape(x.shape)

    token, weight = P("dp", "ep", None, None), P("ep", None, None)
    return jax.shard_map(
        local,
        mesh=mesh,
        in_specs=(token,) * 4 + (weight,) * 3,
        out_specs=token,
        check_vma=False,
    )
```

```python
import functools

import jax
import jax.numpy as jnp
from jax import lax
from jax.experimental import pallas as pl
from jax.experimental.pallas import tpu as pltpu
from jax.sharding import PartitionSpec as P

MESH = pl.DeviceIdType.MESH
F32, BF16 = jnp.float32, jnp.bfloat16
GROUPS = ((0,), (1,), (2,), (3,), (4,), (5,), (6,), (7,))
STEP = 4
AHEAD = 2


def kernel(
    n, slots, width,
    x_hbm, ex, sl, ga, wg_hbm, wu_hbm, wd_hbm, y_hbm,
    xall, accg, accu, z, h, disp, comb, wgb, wub, wdb, me_c, me_g, pr, r1, r2,
    x_sem, wg_sem, wu_sem, wd_sem, y_sem, ms_sem, mr_sem, as_sem, ar_sem, ss_sem, sr_sem,
):
    experts = wg_hbm.shape[0]
    tokens = x_hbm.shape[0]
    ff = wg_hbm.shape[2]
    top = ex.shape[0]
    rows = experts * slots
    chunks = xall.shape[0]
    half = tokens // 2
    chips = n // 2
    me = lax.axis_index("ep")
    chip, core = me // 2, me % 2
    other = 1 - core
    lchip, rchip, ochip = (chip + chips - 1) % chips, (chip + 1) % chips, (chip + 2) % chips
    left, right, opp, partner = 2 * lchip + core, 2 * rchip + core, 2 * ochip + core, 2 * chip + other
    others = tuple(2 * q + other for q in (chip, lchip, rchip, ochip))

    def rcopy(src, dst, ssem, rsem, dev):
        return pltpu.make_async_remote_copy(
            src_ref=src, dst_ref=dst, send_sem=ssem, recv_sem=rsem,
            device_id={"ep": dev}, device_id_type=MESH,
        )

    def go(copies):
        for c in copies:
            c.start()

    def got(dst, sem):
        rcopy(dst, dst, sem, sem, partner).wait_recv()

    def xload(j):
        return pltpu.make_async_copy(x_hbm.at[:, pl.ds(j * width, width)], xall.at[j, me], x_sem.at[j])

    go([xload(j) for j in range(chunks)])

    def wload(g, e):
        k0, kk = GROUPS[g][0] * width, len(GROUPS[g]) * width
        return [
            pltpu.make_async_copy(
                w.at[e, pl.ds(k0, kk), :], b.at[e, pl.ds(0, kk), :], s.at[e]
            )
            for w, b, s in ((wg_hbm, wgb, wg_sem), (wu_hbm, wub, wu_sem))
        ]

    def dload(r, e):
        cols = pl.ds(pl.multiple_of(r * 2 * width, width), 2 * width)
        return pltpu.make_async_copy(wd_hbm.at[e, :, cols], wdb.at[e], wd_sem.at[e])

    for e in range(experts):
        go(wload(0, e))
    go([dload(0, e) for e in range(experts)])

    barrier = pltpu.get_barrier_semaphore()
    for p in (left, right, partner):
        pl.semaphore_signal(barrier, inc=1, device_id={"ep": p}, device_id_type=MESH)
    me_c[me] = jnp.where(sl[...] < slots, ex[...] * slots + sl[...], -1)
    me_g[me] = ga[...]
    pl.semaphore_wait(barrier, 3)

    def table(i, r, s, dev):
        return [
            rcopy(t.at[s], t.at[s], ms_sem.at[k, i], mr_sem.at[k, r], dev) for k, t in enumerate((me_c, me_g))
        ]

    def tgot(r, s):
        for k, t in enumerate((me_c, me_g)):
            got(t.at[s], mr_sem.at[k, r])

    t_own = table(0, 0, me, right) + table(1, 1, me, left) + table(2, 4, me, partner)
    t_next = table(3, 2, left, right) + table(4, 5, left, partner) + table(5, 6, right, partner)
    t_last = table(6, 7, opp, partner)

    def own(j):
        return [
            rcopy(xall.at[j, me], xall.at[j, me], as_sem.at[0, j], ar_sem.at[0, j], right),
            rcopy(xall.at[j, me], xall.at[j, me], as_sem.at[1, j], ar_sem.at[1, j], left),
            rcopy(xall.at[j, me], xall.at[j, me], as_sem.at[2, j], ar_sem.at[4, j], partner),
        ]

    lo, hi = pl.ds(0, half), pl.ds(half, half)

    def forward(j):
        return [
            rcopy(xall.at[j, left, lo], xall.at[j, left, lo], as_sem.at[3, j], ar_sem.at[2, j], right),
            rcopy(xall.at[j, right, hi], xall.at[j, right, hi], as_sem.at[4, j], ar_sem.at[3, j], left),
            rcopy(xall.at[j, left], xall.at[j, left], as_sem.at[5, j], ar_sem.at[5, j], partner),
            rcopy(xall.at[j, right], xall.at[j, right], as_sem.at[6, j], ar_sem.at[6, j], partner),
        ]

    def across(j):
        return [rcopy(xall.at[j, opp], xall.at[j, opp], as_sem.at[7, j], ar_sem.at[7, j], partner)]

    def send_own(j):
        xload(j).wait()
        go(own(j))

    def step_a(j):
        got(xall.at[j, left], ar_sem.at[0, j])
        got(xall.at[j, right], ar_sem.at[1, j])
        go(forward(j))
        if j + AHEAD < chunks:
            send_own(j + AHEAD)

    def step_b(j):
        got(xall.at[j, opp, lo], ar_sem.at[2, j])
        got(xall.at[j, opp, hi], ar_sem.at[3, j])
        go(across(j))

    def step_c(j):
        for i, s in enumerate(others):
            got(xall.at[j, s], ar_sem.at[4 + i, j])

    A, B = (functools.partial(functools.partial, f) for f in (step_a, step_b))

    go(t_own)
    for j in range(AHEAD):
        send_own(j)
    tgot(0, left)
    tgot(1, right)
    go(t_next)
    tgot(2, opp)
    go(t_last)
    step_a(0)
    for i, s in enumerate(others):
        tgot(4 + i, s)

    def tables(s, _):
        code, g = me_c[s] - rows * me, me_g[s]
        for r0 in range(0, rows, 128):
            size = min(128, rows - r0)
            row = r0 + lax.broadcasted_iota(jnp.int32, (size, tokens), 0)
            w = jnp.zeros((size, tokens), F32)
            d = jnp.zeros((size, tokens), F32)
            for k in range(top):
                hit = row == code[k : k + 1, :]
                w = jnp.where(hit, g[k : k + 1, :], w)
                d = jnp.where(hit, 1.0, d)
            disp[s, r0 : r0 + size, :] = d.astype(BF16)
            comb[s, :, r0 : r0 + size] = w.T.astype(BF16)
        return _

    lax.fori_loop(0, n - 2, tables, 0)
    step_a(1)
    lax.fori_loop(n - 2, n, tables, 0)

    def dispatch(j, k0):
        for q in range(chips):
            a = jnp.dot(disp[2 * q], xall[j, 2 * q], preferred_element_type=F32)
            b = jnp.dot(disp[2 * q + 1], xall[j, 2 * q + 1], preferred_element_type=F32)
            at = slice(q * 2 * slots, (q + 1) * 2 * slots)
            for e in range(experts):
                part = slice(e * slots, (e + 1) * slots)
                z[e, at, k0 : k0 + width] = jnp.concatenate([a[part], b[part]], 0).astype(BF16)

    def gemm1(g, hooks):
        kk = len(GROUPS[g]) * width
        first, last = g == 0, g == len(GROUPS) - 1

        def pair(p, _):
            for at, hook in hooks:
                pl.when(p == at)(hook)
            es = [STEP * p + i for i in range(STEP)]
            for e in es:
                for c in wload(g, e):
                    c.wait()
            for e in es:
                lhs = z[e, :, :kk]
                for f0 in range(0, ff, width):
                    f = slice(f0, f0 + width)
                    gg = jnp.dot(lhs, wgb[e, :kk, f], preferred_element_type=F32)
                    uu = jnp.dot(lhs, wub[e, :kk, f], preferred_element_type=F32)
                    if not first:
                        gg += accg[e, :, f]
                        uu += accu[e, :, f]
                    if last:
                        h[e, :, f] = (gg * jax.nn.sigmoid(gg) * uu).astype(BF16)
                    else:
                        accg[e, :, f] = gg
                        accu[e, :, f] = uu
            if not last:
                for e in es:
                    go(wload(g + 1, e))
            return _

        lax.fori_loop(0, experts // STEP, pair, 0)

    def within(j):
        return [(at, f(k)) for at, f, k in ((1, A, j + 2), (1, B, j + 1)) if k < chunks]

    for g, js in enumerate(GROUPS):
        for i, j in enumerate(js):
            if j == 0:
                step_b(0)
            step_c(j)
            dispatch(j, i * width)
        gemm1(g, within(js[0]))

    for c in t_own + t_next + t_last:
        c.wait_send()
    for j in range(chunks):
        for c in own(j) + forward(j) + across(j):
            c.wait_send()

    keep = lambda c, q: accg.at[c, pl.ds(0, tokens), pl.ds(pl.multiple_of(q * width, width), width)]

    def die(c):
        return rcopy(xall.at[c, pl.ds(0, chips)], pr.at[c], ss_sem.at[0, c], sr_sem.at[0, c], partner)

    def far(c):
        return [
            rcopy(xall.at[c, chips, lo], r1.at[c, 0], ss_sem.at[1, c], sr_sem.at[1, c], right),
            rcopy(xall.at[c, chips, hi], r1.at[c, 1], ss_sem.at[2, c], sr_sem.at[2, c], left),
        ]

    def near(c):
        return [
            rcopy(xall.at[c, chips + 1, hi], r2.at[c, 0, hi], ss_sem.at[3, c], sr_sem.at[3, c], right),
            rcopy(xall.at[c, chips + 2, lo], r2.at[c, 1, lo], ss_sem.at[4, c], sr_sem.at[4, c], left),
        ]

    def merged(c):
        return [
            rcopy(xall.at[c, chips + 1, lo], r2.at[c, 0, lo], ss_sem.at[5, c], sr_sem.at[5, c], right),
            rcopy(xall.at[c, chips + 2, hi], r2.at[c, 1, hi], ss_sem.at[6, c], sr_sem.at[6, c], left),
        ]

    def store(c):
        return pltpu.make_async_copy(
            xall.at[c, chips + 3], y_hbm.at[:, pl.ds(pl.multiple_of(c * width, width), width)], y_sem.at[c]
        )

    def both(c, q, at):
        return keep(c, q)[at] + pr[c, q, at].astype(F32)

    def stage1(c):
        die(c).wait_recv()
        xall[c, chips] = both(c, ochip, pl.ds(0, tokens)).astype(BF16)
        xall[c, chips + 1, hi] = both(c, rchip, hi).astype(BF16)
        xall[c, chips + 2, lo] = both(c, lchip, lo).astype(BF16)
        go(far(c) + near(c))

    def stage2(c):
        for k in far(c):
            k.wait_recv()
        xall[c, chips + 1, lo] = (both(c, rchip, lo) + r1[c, 0].astype(F32)).astype(BF16)
        xall[c, chips + 2, hi] = (both(c, lchip, hi) + r1[c, 1].astype(F32)).astype(BF16)
        go(merged(c))

    def stage3(c):
        for k in near(c) + merged(c):
            k.wait_recv()
        total = both(c, chip, pl.ds(0, tokens)) + r2[c, 0].astype(F32) + r2[c, 1].astype(F32)
        xall[c, chips + 3] = total.astype(BF16)
        store(c).start()

    def down(r, k, within, last):
        c = 2 * r + k
        col = slice(k * width, (k + 1) * width)
        for i in range(experts // 2):
            if i % 2 == 0 and k == 0:
                for e in range(2 * i, 2 * i + 4):
                    dload(r, e).wait()
            pieces = [
                jnp.dot(h[e], wdb[e, :, col], preferred_element_type=F32) for e in (2 * i, 2 * i + 1)
            ]
            at = slice(i * 2 * slots, (i + 1) * 2 * slots)
            for s in range(n):
                part = slice(s * slots, (s + 1) * slots)
                z[s, at, :width] = jnp.concatenate([v[part] for v in pieces], 0).astype(BF16)
            if i % 2:
                if k == 1:
                    pl.when(r + 1 < chunks // 2)(lambda: go([dload(r + 1, e) for e in range(2 * i - 2, 2 * i + 2)]))
                (within if i == 1 else last)(c)
        for q in range(chips):
            s = 2 * q + other
            xall[c, q] = jnp.dot(comb[s], z[s, :, :width], preferred_element_type=F32).astype(BF16)
        die(c).start()
        for q in range(chips):
            s = 2 * q + core
            keep(c, q)[...] = jnp.dot(comb[s], z[s, :, :width], preferred_element_type=F32)

    def round_(r, _):
        def within(c):
            pl.when(c >= 1)(lambda: stage1(c - 1))

        def last(c):
            pl.when(c >= 2)(lambda: stage2(c - 2))
            pl.when(c >= 4)(lambda: stage3(c - 4))

        down(r, 0, within, last)
        down(r, 1, within, last)
        return _

    lax.fori_loop(0, chunks // 2, round_, 0)
    c = chunks - 1
    for f, k in ((stage1, 0), (stage2, 1), (stage3, 3), (stage2, 0), (stage3, 2), (stage3, 1), (stage3, 0)):
        f(c - k)

    def drain(c, _):
        die(c).wait_send()
        for k in far(c) + near(c) + merged(c):
            k.wait_send()
        store(c).wait()
        return _

    lax.fori_loop(0, chunks, drain, 0)


def solution(mesh):
    n = mesh.shape["ep"]

    def local(x, expert, slot, gate, w_gate, w_up, w_down):
        tokens, model = x.shape[2:]
        top = expert.shape[3]
        experts, _, ff = w_gate.shape
        slots = 5 * tokens * top // (4 * experts * n)
        rows = experts * slots
        width = 256
        chunks = model // width
        flat = lambda v: v.reshape(tokens, top).T
        vmem = pltpu.VMEM
        dma = pltpu.SemaphoreType.DMA
        any_, inv = pl.BlockSpec(memory_space=pl.ANY), pl.BlockSpec(memory_space=pltpu.VMEM)
        flops = 6 * n * rows * model * ff
        y = pl.pallas_call(
            functools.partial(kernel, n, slots, width),
            out_shape=jax.ShapeDtypeStruct((tokens, model), BF16),
            in_specs=[any_, inv, inv, inv, any_, any_, any_],
            out_specs=any_,
            scratch_shapes=[
                vmem((chunks, n, tokens, width), BF16),
                vmem((experts, n * slots, ff), F32),
                vmem((experts, n * slots, ff), F32),
                vmem((n, rows, width), BF16),
                vmem((experts, n * slots, ff), BF16),
                vmem((n, rows, tokens), BF16),
                vmem((n, tokens, rows), BF16),
                vmem((experts, width, ff), BF16),
                vmem((experts, width, ff), BF16),
                vmem((experts, ff, 2 * width), BF16),
                vmem((n, top, tokens), jnp.int32),
                vmem((n, top, tokens), F32),
                vmem((chunks, n // 2, tokens, width), BF16),
                vmem((chunks, 2, tokens // 2, width), BF16),
                vmem((chunks, 2, tokens, width), BF16),
                dma((chunks,)),
                dma((experts,)),
                dma((experts,)),
                dma((experts,)),
                dma((chunks,)),
                dma((2, 7)),
                dma((2, 8)),
                dma((8, chunks)),
                dma((8, chunks)),
                dma((7, chunks)),
                dma((7, chunks)),
            ],
            compiler_params=pltpu.CompilerParams(
                collective_id=0, has_side_effects=True, vmem_limit_bytes=67_000_000
            ),
            cost_estimate=pl.CostEstimate(
                flops=flops, bytes_accessed=6 * experts * model * ff, transcendentals=n * rows * ff
            ),
            name="moe",
        )(x.reshape(tokens, model), flat(expert), flat(slot), flat(gate), w_gate, w_up, w_down)
        return y.reshape(x.shape)

    token, weight = P("dp", "ep", None, None), P("ep", None, None)
    return jax.shard_map(
        local,
        mesh=mesh,
        in_specs=(token,) * 4 + (weight,) * 3,
        out_specs=token,
        check_vma=False,
    )
```

```python
import functools

import jax
import jax.numpy as jnp
from jax import lax
from jax.experimental import pallas as pl
from jax.experimental.pallas import tpu as pltpu
from jax.sharding import PartitionSpec as P

MESH = pl.DeviceIdType.MESH
F32, BF16 = jnp.float32, jnp.bfloat16
GROUPS = ((0,), (1,), (2,), (3,), (4,), (5,), (6,), (7,))
STEP = 4
AHEAD = 2


def kernel(
    n, slots, width,
    x_hbm, ex, sl, ga, wg_hbm, wu_hbm, wd_hbm, y_hbm,
    xall, accg, accu, z, h, disp, comb, wgb, wub, wdb, me_c, me_g, pr, r1, r2,
    x_sem, wg_sem, wu_sem, wd_sem, y_sem, ms_sem, mr_sem, as_sem, ar_sem, ss_sem, sr_sem,
):
    experts = wg_hbm.shape[0]
    tokens = x_hbm.shape[0]
    ff = wg_hbm.shape[2]
    top = ex.shape[0]
    rows = experts * slots
    chunks = xall.shape[0]
    half = tokens // 2
    chips = n // 2
    me = lax.axis_index("ep")
    chip, core = me // 2, me % 2
    other = 1 - core
    lchip, rchip, ochip = (chip + chips - 1) % chips, (chip + 1) % chips, (chip + 2) % chips
    left, right, opp, partner = 2 * lchip + core, 2 * rchip + core, 2 * ochip + core, 2 * chip + other
    others = tuple(2 * q + other for q in (chip, lchip, rchip, ochip))

    def rcopy(src, dst, ssem, rsem, dev):
        return pltpu.make_async_remote_copy(
            src_ref=src, dst_ref=dst, send_sem=ssem, recv_sem=rsem,
            device_id={"ep": dev}, device_id_type=MESH,
        )

    def go(copies):
        for c in copies:
            c.start()

    def got(dst, sem):
        rcopy(dst, dst, sem, sem, partner).wait_recv()

    def xload(j):
        return pltpu.make_async_copy(x_hbm.at[:, pl.ds(j * width, width)], xall.at[j, me], x_sem.at[j])

    go([xload(j) for j in range(chunks)])

    def wload(g, e):
        k0, kk = GROUPS[g][0] * width, len(GROUPS[g]) * width
        return [
            pltpu.make_async_copy(
                w.at[e, pl.ds(k0, kk), :], b.at[e, pl.ds(0, kk), :], s.at[e]
            )
            for w, b, s in ((wg_hbm, wgb, wg_sem), (wu_hbm, wub, wu_sem))
        ]

    def dload(r, e):
        cols = pl.ds(pl.multiple_of(r * 2 * width, width), 2 * width)
        return pltpu.make_async_copy(wd_hbm.at[e, :, cols], wdb.at[e], wd_sem.at[e])

    for e in range(experts):
        go(wload(0, e))
    go([dload(0, e) for e in range(experts)])

    barrier = pltpu.get_barrier_semaphore()
    for p in (left, right, partner):
        pl.semaphore_signal(barrier, inc=1, device_id={"ep": p}, device_id_type=MESH)
    me_c[me] = jnp.where(sl[...] < slots, ex[...] * slots + sl[...], -1)
    me_g[me] = ga[...]
    pl.semaphore_wait(barrier, 3)

    def table(i, r, s, dev):
        return [
            rcopy(t.at[s], t.at[s], ms_sem.at[k, i], mr_sem.at[k, r], dev) for k, t in enumerate((me_c, me_g))
        ]

    def tgot(r, s):
        for k, t in enumerate((me_c, me_g)):
            got(t.at[s], mr_sem.at[k, r])

    t_own = table(0, 0, me, right) + table(1, 1, me, left) + table(2, 4, me, partner)
    t_next = table(3, 2, left, right) + table(4, 5, left, partner) + table(5, 6, right, partner)
    t_last = table(6, 7, opp, partner)

    lo, hi = pl.ds(0, half), pl.ds(half, half)

    def own(j):
        sends = ((lo, 0, 0, right), (hi, 1, 1, left), (hi, 8, 8, right), (lo, 9, 9, left))
        return [
            rcopy(xall.at[j, me, at], xall.at[j, me, at], as_sem.at[i, j], ar_sem.at[r, j], dev)
            for at, i, r, dev in sends
        ] + [rcopy(xall.at[j, me], xall.at[j, me], as_sem.at[2, j], ar_sem.at[4, j], partner)]

    def forward(j):
        return [
            rcopy(xall.at[j, left, lo], xall.at[j, left, lo], as_sem.at[3, j], ar_sem.at[2, j], right),
            rcopy(xall.at[j, right, hi], xall.at[j, right, hi], as_sem.at[4, j], ar_sem.at[3, j], left),
        ]

    def across(j):
        return [
            rcopy(xall.at[j, s], xall.at[j, s], as_sem.at[i, j], ar_sem.at[i, j], partner)
            for i, s in ((5, left), (6, right), (7, opp))
        ]

    def send_own(j):
        xload(j).wait()
        go(own(j))

    def step_a(j):
        got(xall.at[j, left, lo], ar_sem.at[0, j])
        got(xall.at[j, right, hi], ar_sem.at[1, j])
        go(forward(j))
        if j + AHEAD < chunks:
            send_own(j + AHEAD)

    def step_b(j):
        got(xall.at[j, left, hi], ar_sem.at[8, j])
        got(xall.at[j, right, lo], ar_sem.at[9, j])
        got(xall.at[j, opp, lo], ar_sem.at[2, j])
        got(xall.at[j, opp, hi], ar_sem.at[3, j])
        go(across(j))

    def step_c(j):
        for i, s in enumerate(others):
            got(xall.at[j, s], ar_sem.at[4 + i, j])

    A, B = (functools.partial(functools.partial, f) for f in (step_a, step_b))

    go(t_own)
    for j in range(AHEAD):
        send_own(j)
    tgot(0, left)
    tgot(1, right)
    go(t_next)
    tgot(2, opp)
    go(t_last)
    step_a(0)
    for i, s in enumerate(others):
        tgot(4 + i, s)

    def tables(s, _):
        code, g = me_c[s] - rows * me, me_g[s]
        for r0 in range(0, rows, 128):
            size = min(128, rows - r0)
            row = r0 + lax.broadcasted_iota(jnp.int32, (size, tokens), 0)
            w = jnp.zeros((size, tokens), F32)
            d = jnp.zeros((size, tokens), F32)
            for k in range(top):
                hit = row == code[k : k + 1, :]
                w = jnp.where(hit, g[k : k + 1, :], w)
                d = jnp.where(hit, 1.0, d)
            disp[s, r0 : r0 + size, :] = d.astype(BF16)
            comb[s, :, r0 : r0 + size] = w.T.astype(BF16)
        return _

    lax.fori_loop(0, n - 2, tables, 0)
    step_a(1)
    lax.fori_loop(n - 2, n, tables, 0)

    def dispatch(j, k0):
        for q in range(chips):
            a = jnp.dot(disp[2 * q], xall[j, 2 * q], preferred_element_type=F32)
            b = jnp.dot(disp[2 * q + 1], xall[j, 2 * q + 1], preferred_element_type=F32)
            at = slice(q * 2 * slots, (q + 1) * 2 * slots)
            for e in range(experts):
                part = slice(e * slots, (e + 1) * slots)
                z[e, at, k0 : k0 + width] = jnp.concatenate([a[part], b[part]], 0).astype(BF16)

    def gemm1(g, hooks):
        kk = len(GROUPS[g]) * width
        first, last = g == 0, g == len(GROUPS) - 1

        def pair(p, _):
            for at, hook in hooks:
                pl.when(p == at)(hook)
            es = [STEP * p + i for i in range(STEP)]
            for e in es:
                for c in wload(g, e):
                    c.wait()
            for e in es:
                lhs = z[e, :, :kk]
                for f0 in range(0, ff, width):
                    f = slice(f0, f0 + width)
                    gg = jnp.dot(lhs, wgb[e, :kk, f], preferred_element_type=F32)
                    uu = jnp.dot(lhs, wub[e, :kk, f], preferred_element_type=F32)
                    if not first:
                        gg += accg[e, :, f]
                        uu += accu[e, :, f]
                    if last:
                        h[e, :, f] = (gg * jax.nn.sigmoid(gg) * uu).astype(BF16)
                    else:
                        accg[e, :, f] = gg
                        accu[e, :, f] = uu
            if not last:
                for e in es:
                    go(wload(g + 1, e))
            return _

        lax.fori_loop(0, experts // STEP, pair, 0)

    def within(j):
        return [(at, f(k)) for at, f, k in ((0, A, j + 2), (1, B, j + 1)) if k < chunks]

    for g, js in enumerate(GROUPS):
        for i, j in enumerate(js):
            if j == 0:
                step_b(0)
            step_c(j)
            dispatch(j, i * width)
        gemm1(g, within(js[0]))

    for c in t_own + t_next + t_last:
        c.wait_send()
    for j in range(chunks):
        for c in own(j) + forward(j) + across(j):
            c.wait_send()

    keep = lambda c, q: accg.at[c, pl.ds(0, tokens), pl.ds(pl.multiple_of(q * width, width), width)]

    def die(c):
        return rcopy(xall.at[c, pl.ds(0, chips)], pr.at[c], ss_sem.at[0, c], sr_sem.at[0, c], partner)

    def far(c):
        return [
            rcopy(xall.at[c, chips, lo], r1.at[c, 0], ss_sem.at[1, c], sr_sem.at[1, c], right),
            rcopy(xall.at[c, chips, hi], r1.at[c, 1], ss_sem.at[2, c], sr_sem.at[2, c], left),
        ]

    def near(c):
        return [
            rcopy(xall.at[c, chips + 1, hi], r2.at[c, 0, hi], ss_sem.at[3, c], sr_sem.at[3, c], right),
            rcopy(xall.at[c, chips + 2, lo], r2.at[c, 1, lo], ss_sem.at[4, c], sr_sem.at[4, c], left),
        ]

    def merged(c):
        return [
            rcopy(xall.at[c, chips + 1, lo], r2.at[c, 0, lo], ss_sem.at[5, c], sr_sem.at[5, c], right),
            rcopy(xall.at[c, chips + 2, hi], r2.at[c, 1, hi], ss_sem.at[6, c], sr_sem.at[6, c], left),
        ]

    def store(c):
        return pltpu.make_async_copy(
            xall.at[c, chips + 3], y_hbm.at[:, pl.ds(pl.multiple_of(c * width, width), width)], y_sem.at[c]
        )

    def both(c, q, at):
        return keep(c, q)[at] + pr[c, q, at].astype(F32)

    def stage1(c):
        die(c).wait_recv()
        xall[c, chips] = both(c, ochip, pl.ds(0, tokens)).astype(BF16)
        xall[c, chips + 1, hi] = both(c, rchip, hi).astype(BF16)
        xall[c, chips + 2, lo] = both(c, lchip, lo).astype(BF16)
        go(far(c) + near(c))

    def stage2(c):
        for k in far(c):
            k.wait_recv()
        xall[c, chips + 1, lo] = (both(c, rchip, lo) + r1[c, 0].astype(F32)).astype(BF16)
        xall[c, chips + 2, hi] = (both(c, lchip, hi) + r1[c, 1].astype(F32)).astype(BF16)
        go(merged(c))

    def stage3(c):
        for k in near(c) + merged(c):
            k.wait_recv()
        total = both(c, chip, pl.ds(0, tokens)) + r2[c, 0].astype(F32) + r2[c, 1].astype(F32)
        xall[c, chips + 3] = total.astype(BF16)
        store(c).start()

    def down(r, k, within, last):
        c = 2 * r + k
        col = slice(k * width, (k + 1) * width)
        for i in range(experts // 2):
            if i % 2 == 0 and k == 0:
                for e in range(2 * i, 2 * i + 4):
                    dload(r, e).wait()
            pieces = [
                jnp.dot(h[e], wdb[e, :, col], preferred_element_type=F32) for e in (2 * i, 2 * i + 1)
            ]
            at = slice(i * 2 * slots, (i + 1) * 2 * slots)
            for s in range(n):
                part = slice(s * slots, (s + 1) * slots)
                z[s, at, :width] = jnp.concatenate([v[part] for v in pieces], 0).astype(BF16)
            if i % 2:
                if k == 1:
                    pl.when(r + 1 < chunks // 2)(lambda: go([dload(r + 1, e) for e in range(2 * i - 2, 2 * i + 2)]))
                (within if i == 1 else last)(c)
        for q in range(chips):
            s = 2 * q + other
            xall[c, q] = jnp.dot(comb[s], z[s, :, :width], preferred_element_type=F32).astype(BF16)
        die(c).start()
        for q in range(chips):
            s = 2 * q + core
            keep(c, q)[...] = jnp.dot(comb[s], z[s, :, :width], preferred_element_type=F32)

    def round_(r, _):
        def within(c):
            pl.when(c >= 1)(lambda: stage1(c - 1))

        def last(c):
            pl.when(c >= 2)(lambda: stage2(c - 2))
            pl.when(c >= 4)(lambda: stage3(c - 4))

        down(r, 0, within, last)
        down(r, 1, within, last)
        return _

    lax.fori_loop(0, chunks // 2, round_, 0)
    c = chunks - 1
    for f, k in ((stage1, 0), (stage2, 1), (stage3, 3), (stage2, 0), (stage3, 2), (stage3, 1), (stage3, 0)):
        f(c - k)

    def drain(c, _):
        die(c).wait_send()
        for k in far(c) + near(c) + merged(c):
            k.wait_send()
        store(c).wait()
        return _

    lax.fori_loop(0, chunks, drain, 0)


def solution(mesh):
    n = mesh.shape["ep"]

    def local(x, expert, slot, gate, w_gate, w_up, w_down):
        tokens, model = x.shape[2:]
        top = expert.shape[3]
        experts, _, ff = w_gate.shape
        slots = 5 * tokens * top // (4 * experts * n)
        rows = experts * slots
        width = 256
        chunks = model // width
        flat = lambda v: v.reshape(tokens, top).T
        vmem = pltpu.VMEM
        dma = pltpu.SemaphoreType.DMA
        any_, inv = pl.BlockSpec(memory_space=pl.ANY), pl.BlockSpec(memory_space=pltpu.VMEM)
        flops = 6 * n * rows * model * ff
        y = pl.pallas_call(
            functools.partial(kernel, n, slots, width),
            out_shape=jax.ShapeDtypeStruct((tokens, model), BF16),
            in_specs=[any_, inv, inv, inv, any_, any_, any_],
            out_specs=any_,
            scratch_shapes=[
                vmem((chunks, n, tokens, width), BF16),
                vmem((experts, n * slots, ff), F32),
                vmem((experts, n * slots, ff), F32),
                vmem((n, rows, width), BF16),
                vmem((experts, n * slots, ff), BF16),
                vmem((n, rows, tokens), BF16),
                vmem((n, tokens, rows), BF16),
                vmem((experts, width, ff), BF16),
                vmem((experts, width, ff), BF16),
                vmem((experts, ff, 2 * width), BF16),
                vmem((n, top, tokens), jnp.int32),
                vmem((n, top, tokens), F32),
                vmem((chunks, n // 2, tokens, width), BF16),
                vmem((chunks, 2, tokens // 2, width), BF16),
                vmem((chunks, 2, tokens, width), BF16),
                dma((chunks,)),
                dma((experts,)),
                dma((experts,)),
                dma((experts,)),
                dma((chunks,)),
                dma((2, 7)),
                dma((2, 8)),
                dma((10, chunks)),
                dma((10, chunks)),
                dma((7, chunks)),
                dma((7, chunks)),
            ],
            compiler_params=pltpu.CompilerParams(
                collective_id=0, has_side_effects=True, vmem_limit_bytes=67_000_000
            ),
            cost_estimate=pl.CostEstimate(
                flops=flops, bytes_accessed=6 * experts * model * ff, transcendentals=n * rows * ff
            ),
            name="moe",
        )(x.reshape(tokens, model), flat(expert), flat(slot), flat(gate), w_gate, w_up, w_down)
        return y.reshape(x.shape)

    token, weight = P("dp", "ep", None, None), P("ep", None, None)
    return jax.shard_map(
        local,
        mesh=mesh,
        in_specs=(token,) * 4 + (weight,) * 3,
        out_specs=token,
        check_vma=False,
    )
```
